128 devices in a mesh: data: 1, model: 2 (over core), time: 64 (over z, y, x).
Axes of the slice: x: 4, y: 4, z: 4, core: 2. Of those that a mesh axis runs over, the one named last changes fastest.
Arguments:
- x_init: float32 [4, 4096, 16], P('data')
- w_up: bfloat16 [16, 1152], P(None, 'model')
- w_down: bfloat16 [1152, 16], P('model')
- mod_scale: bfloat16 [384, 1152], P('time', 'model')
- mod_shift: bfloat16 [384, 1152], P('time', 'model')
- step_size: float32 [384], P('time')
Outputs:
- output: float32 [384, 4, 4096, 16], P('time', 'data')
All inputs are finite; a program needn't handle non-finite values.
Results may differ from the reference program's by a relative error of at most 0.001.
Values are sent between devices in bfloat16 or wider.
A program may use at most 1 GiB of HBM per device.

```python
import jax
import jax.numpy as jnp
from jax import lax

STEPS = 384
BATCH = 4
TOKENS = 4096
CHAN = 16
HIDDEN = 1152
SWEEPS = 4


def setup_inputs(seed: int = 0, part: int = 0) -> dict:
    base_key = jax.random.key(seed)
    key_list = jax.random.split(base_key, 6)
    part_key = jax.random.fold_in(key_list[5], part)
    x_init = jax.random.normal(part_key, (BATCH, TOKENS, CHAN), jnp.float32)
    w_up = (jax.random.normal(key_list[0], (CHAN, HIDDEN), jnp.float32) * CHAN ** -0.5).astype(jnp.bfloat16)
    w_down = (jax.random.normal(key_list[1], (HIDDEN, CHAN), jnp.float32) * HIDDEN ** -0.5).astype(jnp.bfloat16)
    mod_scale = (0.5 * jax.random.normal(key_list[2], (STEPS, HIDDEN), jnp.float32)).astype(jnp.bfloat16)
    mod_shift = (0.5 * jax.random.normal(key_list[3], (STEPS, HIDDEN), jnp.float32)).astype(jnp.bfloat16)
    step_size = (3.0 / STEPS) * jax.random.uniform(key_list[4], (STEPS,), jnp.float32, 0.2, 1.8)
    return {'x_init': x_init, 'w_up': w_up, 'w_down': w_down, 'mod_scale': mod_scale, 'mod_shift': mod_shift, 'step_size': step_size}


def drift_at(latent, scale_row, shift_row, step_val, w_up, w_down):
    flat_lat = latent.reshape(BATCH * TOKENS, CHAN).astype(jnp.bfloat16)
    pre_act = jnp.dot(flat_lat, w_up, preferred_element_type=jnp.float32)
    hidden = jax.nn.gelu(pre_act * (1.0 + scale_row.astype(jnp.float32)) + shift_row.astype(jnp.float32), approximate=True)
    proj_out = jnp.dot(hidden.astype(jnp.bfloat16), w_down, preferred_element_type=jnp.float32)
    return step_val * proj_out.reshape(BATCH, TOKENS, CHAN)


def reference(x_init, w_up, w_down, mod_scale, mod_shift, step_size):
    def drift_step(packed):
        return drift_at(packed[0], packed[1], packed[2], packed[3], w_up, w_down)

    def one_sweep(latents, unused):
        drifts = lax.map(drift_step, (latents, mod_scale, mod_shift, step_size))
        prefix = jnp.cumsum(drifts, axis=0) - drifts
        return x_init[None] + prefix, unused

    start_lat = jnp.broadcast_to(x_init[None], (STEPS, BATCH, TOKENS, CHAN))
    final_lat, unused = lax.scan(one_sweep, start_lat, None, length=SWEEPS)
    return final_lat
```

```python
import functools
import math

import jax
import jax.numpy as jnp
from jax import lax
from jax.experimental import pallas as pl
from jax.experimental.pallas import tpu as pltpu
from jax.sharding import PartitionSpec as P

MESH = pl.DeviceIdType.MESH
BF = jnp.bfloat16
F32 = jnp.float32
CHIPS = 64
SB = 6
HID = 1152
HALF = 640
TOK = 128
GC = math.sqrt(2.0 / math.pi)
G1 = 2.0 * GC
G2 = 8.0 * 0.044715 * GC
CW = 384


def half_gelu(v):
    return v * jnp.tanh(v * (G1 + G2 * (v * v))) + v


def shift_chip(t, k, sign):
    out = 0
    for unit in (16, 4, 1):
        a = (t // unit) % 4
        b = (k // unit) % 4
        out = out + unit * ((a + sign * b + 4) % 4)
    return out


def main_kernel(mods, steps, wts, x0_hbm, r_out, base_out, lhs_hbm,
                gat, hst, wgt, x0, w1, w2, lh, rx, pre, act, fbuf, bas, run,
                gsem, hsem, wsem, gsend, hsend, wsend, xsem, osem, lsem, fsend, fsib, bsend, bsib, rsem, bsem):
    t = lax.axis_index('time')
    p = lax.axis_index('model')
    q = 1 - p
    blk = t * 2 + p
    row = blk // 32
    col = pl.multiple_of((blk % 32) * TOK, TOK)

    def dev(tt, pp):
        return {'time': tt, 'model': pp}

    cp_x = pltpu.make_async_copy(x0_hbm.at[row, :, pl.ds(col, TOK)], x0, xsem)
    cp_x.start()
    pltpu.make_async_copy(mods, gat.at[0, p], gsem.at[0]).start()
    pltpu.make_async_copy(steps, hst.at[0], hsem.at[0]).start()
    pltpu.make_async_copy(wts, wgt.at[p], wsem).start()
    cp_w = pltpu.make_async_remote_copy(wts, wgt.at[p], wsend, wsem, device_id=dev(t, q), device_id_type=MESH)
    cp_w.start()
    cp_g0 = pltpu.make_async_remote_copy(mods, gat.at[0, p], gsend.at[0], gsem.at[0], device_id=dev(t, q), device_id_type=MESH)
    cp_g0.start()

    def send_mods(k, carry):
        d = shift_chip(t, k, -1)
        for c in range(2):
            pltpu.make_async_remote_copy(mods, gat.at[k, p], gsend.at[k], gsem.at[k], device_id=dev(d, c), device_id_type=MESH).start()
        pltpu.make_async_remote_copy(steps, hst.at[k], hsend.at[k], hsem.at[k], device_id=dev(d, p), device_id_type=MESH).start()
        return carry

    lax.fori_loop(1, CHIPS, send_mods, 0)

    zero = jnp.zeros((16, TOK), BF)
    ones_row = jnp.where(lax.broadcasted_iota(jnp.int32, (16, TOK), 0) == 0, 1.0, 0.0).astype(BF)
    for pr in range(3):
        for r in range(8):
            for m in range(2):
                rx[pr, 16 * r:16 * r + 16, TOK * m:TOK * m + TOK] = ones_row if r == 4 * m + 3 else zero
    act[1] = jnp.zeros(act.shape[1:], BF)
    pltpu.make_async_copy(wgt, wgt, wsem).wait()
    wf = wgt[...].astype(F32)

    def merged(a, b):
        return jnp.concatenate([a[:, :512], b[:, :512], a[:, 512:] + b[:, 512:]], axis=1)

    w1[...] = merged(wf[0, :16], wf[1, :16])
    w2[...] = merged(wf[0, 16:], wf[1, 16:]).astype(BF)
    cp_x.wait()

    first = lax.broadcasted_iota(jnp.int32, (16, HID), 0) == 0

    def build(k, slot):
        mf = merged(gat[k, 0].astype(F32), gat[k, 1].astype(F32))
        w = w1[...]
        for pr in range(3):
            parts = []
            for m in range(2):
                j = 2 * pr + m
                ws = w * (0.5 * mf[j:j + 1] + 0.5)
                hi = ws.astype(BF)
                rest = ws - hi.astype(F32)
                mid = rest.astype(BF)
                low = (rest - mid.astype(F32)).astype(BF)
                bias = jnp.where(first, 0.5 * mf[SB + j:SB + j + 1], 0.0).astype(BF)
                parts += [hi, mid, low, bias]
            full = jnp.concatenate(parts, axis=0)
            for c in range(0, HID, 128):
                lh[slot, pr, c:c + 128, :] = full[:, c:c + 128].T

    def put_x(j, x):
        xb = x.astype(BF)
        pr, m = j // 2, j % 2
        for r in range(3):
            rx[pr, 64 * m + 16 * r:64 * m + 16 * r + 16, TOK * m:TOK * m + TOK] = xb

    def rx_prefix(s, c):
        for j in range(SB):
            put_x(j, s)
            s = s + fbuf[c, j]
        return s

    def body(cur, slot, finish):
        def mm1(pr, lo):
            pre[1 - cur, pr, lo:lo + CW, :] = jnp.dot(lh[slot, pr, lo:lo + CW, :], rx[pr], preferred_element_type=F32)
        rows = []
        for pr in range(3):
            acc = jnp.zeros((16, 2 * TOK), F32)
            for lo in range(0, HID, CW):
                mm1(pr, lo)
                acc = acc + jnp.dot(w2[:, lo:lo + CW], act[1 - cur, pr, lo:lo + CW, :], preferred_element_type=F32)
                act[cur, pr, lo:lo + CW, :] = half_gelu(pre[cur, pr, lo:lo + CW, :]).astype(BF)
            rows += [acc[:, :TOK], acc[:, TOK:]]
        finish(rows)

    def tail(cur, finish):
        rows = []
        for pr in range(3):
            acc = jnp.dot(w2[...], act[cur, pr], preferred_element_type=F32)
            rows += [acc[:, :TOK], acc[:, TOK:]]
        finish(rows)

    def head(slot):
        for pr in range(3):
            for lo in range(0, HID, CW):
                pre[0, pr, lo:lo + CW, :] = jnp.dot(lh[slot, pr, lo:lo + CW, :], rx[pr], preferred_element_type=F32)

    def store_f(c, kk, rows):
        tot = None
        for j in range(SB):
            f = hst[kk, j:j + 1, :] * rows[j]
            fbuf[c, j] = f
            tot = f if tot is None else tot + f
        return tot

    def wait_mods(k):
        pltpu.make_async_copy(gat.at[k], gat.at[k], gsem.at[k]).wait()
        pltpu.make_async_copy(hst.at[k], hst.at[k], hsem.at[k]).wait()

    def out_lh(k):
        return pltpu.make_async_copy(lh.at[k % 4], lhs_hbm.at[shift_chip(t, k, 1)], osem.at[k % 4])

    wait_mods(0)
    build(0, 0)
    wait_mods(1)
    build(1, 1)
    for j in range(SB):
        put_x(j, x0[...])
    head(0)
    out_lh(0).start()

    def sweep0(i, carry):
        for u in range(2):
            n = 2 * i + u

            @pl.when(n + 1 < CHIPS)
            def _():
                out_lh(n + 1).start()

            @pl.when(n + 2 < CHIPS)
            def _():
                wait_mods(n + 2)

            @pl.when((n >= 2) & (n + 2 < CHIPS))
            def _():
                out_lh(n - 2).wait()

            nb = jnp.minimum(n + 2, CHIPS - 1)
            build(nb, jnp.where(n + 2 < CHIPS, (n + 2) % 4, 4))
            prev = jnp.maximum(n - 1, 0)
            where = jnp.where(n == 0, CHIPS, shift_chip(t, prev, 1))
            body(u, jnp.where(n + 1 < CHIPS, (n + 1) % 4, 4), lambda rows: store_f(where, prev, rows))
        return carry

    lax.fori_loop(0, CHIPS // 2, sweep0, 0)
    tail(1, lambda rows: store_f(shift_chip(t, CHIPS - 1, 1), CHIPS - 1, rows))
    for k in range(CHIPS - 4, CHIPS):
        out_lh(k).wait()

    def block_of(s, n):
        if s < 3:
            return n
        return shift_chip(t, (n + 1) % CHIPS, 1)

    def in_lh(s, n, slot):
        return pltpu.make_async_copy(lhs_hbm.at[block_of(s, n)], lh.at[slot], lsem.at[slot])

    for n in range(3):
        in_lh(1, n, n).start()

    for s in (1, 2, 3):
        in_lh(s, 0, 0).wait()
        if s < 3:
            run[0] = rx_prefix(x0[...], 0)
        else:
            rx_prefix(bas[block_of(3, 0)], block_of(3, 0))
        head(0)

        def sweep(i, carry, s=s):
            for u in range(2):
                n = 2 * i + u
                slot = jnp.where(n + 1 < CHIPS, (n + 1) % 4, 4)
                nx = jnp.minimum(n + 1, CHIPS - 1)
                prev = jnp.maximum(n - 1, 0)

                @pl.when(n + 1 < CHIPS)
                def _():
                    in_lh(s, n + 1, (n + 1) % 4).wait()

                @pl.when(n + 3 < CHIPS)
                def _():
                    in_lh(s, n + 3, (n + 3) % 4).start()
                if s < 3:
                    @pl.when(n + 3 >= CHIPS)
                    def _():
                        in_lh(s + 1, n + 3 - CHIPS, (n + 3) % 4).start()
                else:
                    @pl.when(n >= 2)
                    def _():
                        send_f(n - 1)

                if s < 3:
                    run[0] = rx_prefix(run[0], nx)
                else:
                    cn = block_of(3, nx)
                    rx_prefix(bas[cn], cn)
                cp = block_of(s, prev)
                where = jnp.where(n == 0, CHIPS, cp)
                kk = shift_chip(cp, t, -1)

                def finish(rows):
                    tot = store_f(where, kk, rows)
                    if s == 2:
                        bas[where] = run[1]
                        run[1] = jnp.where(n == 0, x0[...], run[1] + tot)
                    if s == 3:
                        bas[where] = tot
                body(u, slot, finish)
            return carry

        def send_f(k):
            c = shift_chip(t, k, 1)
            for pp in range(2):
                pltpu.make_async_remote_copy(fbuf.at[c, pl.ds(0, SB - 1)], r_out.at[:, row, :, pl.ds(col, TOK)],
                                             fsend.at[k], rsem, device_id=dev(c, pp), device_id_type=MESH).start()

        lax.fori_loop(0, CHIPS // 2, sweep, 0)

        last = block_of(s, CHIPS - 1)

        def finish_last(rows, s=s, last=last):
            tot = store_f(last, shift_chip(last, t, -1) if s < 3 else 0, rows)
            if s == 2:
                bas[last] = run[1]
            if s == 3:
                bas[last] = tot
        tail(1, finish_last)

    send_f(CHIPS - 1)
    own_f = pltpu.make_async_copy(fbuf.at[t, pl.ds(0, SB - 1)], r_out.at[:, row, :, pl.ds(col, TOK)], rsem)

    def scan_base(c, s):
        tot = bas[c]
        bas[c] = s
        return s + tot

    lax.fori_loop(0, CHIPS, scan_base, x0[...])

    def send_b(k, carry):
        c = shift_chip(t, k, 1)
        for pp in range(2):
            pltpu.make_async_remote_copy(bas.at[c], base_out.at[row, :, pl.ds(col, TOK)],
                                         bsend.at[k], bsem, device_id=dev(c, pp), device_id_type=MESH).start()
        return carry

    lax.fori_loop(1, CHIPS, send_b, 0)
    own_f.start()
    sib_f = pltpu.make_async_remote_copy(fbuf.at[t, pl.ds(0, SB - 1)], r_out.at[:, row, :, pl.ds(col, TOK)],
                                         fsib, rsem, device_id=dev(t, q), device_id_type=MESH)
    sib_f.start()
    pltpu.make_async_copy(bas.at[t], base_out.at[row, :, pl.ds(col, TOK)], bsem).start()
    sib_b = pltpu.make_async_remote_copy(bas.at[t], base_out.at[row, :, pl.ds(col, TOK)],
                                         bsib, bsem, device_id=dev(t, q), device_id_type=MESH)
    sib_b.start()

    cp_w.wait_send()
    cp_g0.wait_send()

    def drain(k, carry):
        pltpu.make_async_copy(gat.at[k], gat.at[k], gsend.at[k]).wait()
        pltpu.make_async_copy(hst.at[k], hst.at[k], hsend.at[k]).wait()
        pltpu.make_async_copy(fbuf.at[pl.ds(0, 2), pl.ds(0, SB - 1)], fbuf.at[pl.ds(0, 2), pl.ds(0, SB - 1)], fsend.at[k]).wait()
        pltpu.make_async_copy(bas.at[pl.ds(0, 2)], bas.at[pl.ds(0, 2)], bsend.at[k]).wait()
        return carry

    lax.fori_loop(1, CHIPS, drain, 0)
    sib_f.wait_send()
    sib_b.wait_send()
    pltpu.make_async_copy(r_out, r_out, rsem).wait()
    pltpu.make_async_copy(base_out, base_out, bsem).wait()


def sum_kernel(r_ref, b_ref, o_ref):
    s = b_ref[...]
    o_ref[0] = s
    for j in range(SB - 1):
        s = s + r_ref[j]
        o_ref[j + 1] = s


def solution(mesh):
    def device_body(x_init, w_up, w_down, mod_scale, mod_shift, step_size):
        batch, tokens, chan = x_init.shape
        p = lax.axis_index('model')

        def spread(a):
            tail = a[:, 512:]
            z = jnp.zeros_like(tail)
            last = jnp.where(p == 0, jnp.concatenate([tail, z], axis=1), jnp.concatenate([z, tail], axis=1))
            return jnp.concatenate([a[:, :512], last], axis=1)

        mods = spread(jnp.concatenate([mod_scale, mod_shift, jnp.zeros((4, mod_scale.shape[1]), BF)], axis=0))
        wts = spread(jnp.concatenate([w_up, w_down.T], axis=0))
        steps = jnp.broadcast_to(jnp.concatenate([step_size, jnp.zeros((2,), F32)])[:, None], (8, TOK))
        x0 = jnp.swapaxes(x_init, 1, 2)
        vm = pl.BlockSpec(memory_space=pltpu.VMEM)
        hb = pl.BlockSpec(memory_space=pl.ANY)
        dma = pltpu.SemaphoreType.DMA
        r, base, _ = pl.pallas_call(
            main_kernel,
            out_shape=(
                jax.ShapeDtypeStruct((SB - 1, batch, chan, tokens), F32),
                jax.ShapeDtypeStruct((batch, chan, tokens), F32),
                jax.ShapeDtypeStruct((CHIPS, 3, HID, 128), BF),
            ),
            in_specs=[vm, vm, vm, hb],
            out_specs=(hb, hb, hb),
            scratch_shapes=[
                pltpu.VMEM((CHIPS, 2, 16, HALF), BF),
                pltpu.VMEM((CHIPS, 8, TOK), F32),
                pltpu.VMEM((2, 32, HALF), BF),
                pltpu.VMEM((chan, TOK), F32),
                pltpu.VMEM((chan, HID), F32),
                pltpu.VMEM((chan, HID), BF),
                pltpu.VMEM((5, 3, HID, 128), BF),
                pltpu.VMEM((3, 128, 2 * TOK), BF),
                pltpu.VMEM((2, 3, HID, 2 * TOK), F32),
                pltpu.VMEM((2, 3, HID, 2 * TOK), BF),
                pltpu.VMEM((CHIPS + 1, SB, chan, TOK), F32),
                pltpu.VMEM((CHIPS + 1, chan, TOK), F32),
                pltpu.VMEM((2, chan, TOK), F32),
                dma((CHIPS,)), dma((CHIPS,)), dma, dma((CHIPS,)), dma((CHIPS,)), dma, dma,
                dma((4,)), dma((4,)), dma((CHIPS,)), dma, dma((CHIPS,)), dma, dma, dma,
            ],
            compiler_params=pltpu.CompilerParams(has_side_effects=True, vmem_limit_bytes=60 * 2 ** 20),
            name='sweeps',
        )(mods, steps, wts, x0)
        tile = 1024
        out = pl.pallas_call(
            sum_kernel,
            grid=(batch, tokens // tile),
            out_shape=jax.ShapeDtypeStruct((SB, batch, chan, tokens), F32),
            in_specs=[pl.BlockSpec((SB - 1, None, chan, tile), lambda b, i: (0, b, 0, i)),
                      pl.BlockSpec((None, chan, tile), lambda b, i: (b, 0, i))],
            out_specs=pl.BlockSpec((SB, None, chan, tile), lambda b, i: (0, b, 0, i)),
            name='sums',
        )(r, base)
        return jnp.swapaxes(out, 2, 3)

    return jax.shard_map(device_body, mesh=mesh, in_specs=(P('data', None, None), P(None, 'model'), P('model', None), P('time', 'model'), P('time', 'model'), P('time')), out_specs=P('time', 'data', None, None), check_vma=False)
```

```python
import functools
import math

import jax
import jax.numpy as jnp
from jax import lax
from jax.experimental import pallas as pl
from jax.experimental.pallas import tpu as pltpu
from jax.sharding import PartitionSpec as P

MESH = pl.DeviceIdType.MESH
BF = jnp.bfloat16
F32 = jnp.float32
CHIPS = 64
SB = 6
HID = 1152
HALF = 640
TOK = 128
GC = math.sqrt(2.0 / math.pi)
G1 = 2.0 * GC
G2 = 8.0 * 0.044715 * GC
CW = 384
PAIRS = CHIPS // 2


def half_gelu(v):
    return v * jnp.tanh(v * (G1 + G2 * (v * v))) + v


def shift_chip(t, k, sign):
    out = 0
    for unit in (16, 4, 1):
        a = (t // unit) % 4
        b = (k // unit) % 4
        out = out + unit * ((a + sign * b + 4) % 4)
    return out


def main_kernel(mods, steps, wts, x0_hbm, r_out, base_out, lhs_hbm,
                gat, hst, wgt, x0, w1, w2, lh, rx, pre, act, fbuf, bas, run,
                gsem, hsem, wsem, gsend, hsend, wsend, xsem, osem, lsem, fsend, fsib, bsend, bsib, rsem, bsem):
    t = lax.axis_index('time')
    p = lax.axis_index('model')
    q = 1 - p
    blk = t * 2 + p
    row = blk // 32
    col = pl.multiple_of((blk % 32) * TOK, TOK)

    def dev(tt, pp):
        return {'time': tt, 'model': pp}

    cp_x = pltpu.make_async_copy(x0_hbm.at[row, :, pl.ds(col, TOK)], x0, xsem)
    cp_x.start()
    pltpu.make_async_copy(mods, gat.at[0, p], gsem.at[0]).start()
    pltpu.make_async_copy(steps, hst.at[0], hsem.at[0]).start()
    pltpu.make_async_copy(wts, wgt.at[p], wsem).start()
    cp_w = pltpu.make_async_remote_copy(wts, wgt.at[p], wsend, wsem, device_id=dev(t, q), device_id_type=MESH)
    cp_w.start()
    cp_g0 = pltpu.make_async_remote_copy(mods, gat.at[0, p], gsend.at[0], gsem.at[0], device_id=dev(t, q), device_id_type=MESH)
    cp_g0.start()

    def send_mods(k, carry):
        d = shift_chip(t, k, -1)
        for c in range(2):
            pltpu.make_async_remote_copy(mods, gat.at[k, p], gsend.at[k], gsem.at[k], device_id=dev(d, c), device_id_type=MESH).start()
        pltpu.make_async_remote_copy(steps, hst.at[k], hsend.at[k], hsem.at[k], device_id=dev(d, p), device_id_type=MESH).start()
        return carry

    lax.fori_loop(1, CHIPS, send_mods, 0)

    zero = jnp.zeros((16, TOK), BF)
    ones_row = jnp.where(lax.broadcasted_iota(jnp.int32, (16, TOK), 0) == 0, 1.0, 0.0).astype(BF)
    for b in range(2):
        for pr in range(3):
            for r in range(8):
                for m in range(2):
                    rx[b, pr, 16 * r:16 * r + 16, TOK * m:TOK * m + TOK] = ones_row if r == 4 * m + 3 else zero
    act[1] = jnp.zeros(act.shape[1:], BF)
    pltpu.make_async_copy(wgt, wgt, wsem).wait()
    wf = wgt[...].astype(F32)

    def merged(a, b):
        return jnp.concatenate([a[:, :512], b[:, :512], a[:, 512:] + b[:, 512:]], axis=1)

    w1[...] = merged(wf[0, :16], wf[1, :16])
    w2[...] = merged(wf[0, 16:], wf[1, 16:]).astype(BF)
    cp_x.wait()

    first = lax.broadcasted_iota(jnp.int32, (16, HID), 0) == 0

    def build(k, slot, half):
        mf = merged(gat[k, 0].astype(F32), gat[k, 1].astype(F32))
        w = w1[...]
        for pr in range(3):
            parts = []
            for m in range(2):
                j = 2 * pr + m
                ws = w * (0.5 * mf[j:j + 1] + 0.5)
                hi = ws.astype(BF)
                rest = ws - hi.astype(F32)
                mid = rest.astype(BF)
                low = (rest - mid.astype(F32)).astype(BF)
                bias = jnp.where(first, 0.5 * mf[SB + j:SB + j + 1], 0.0).astype(BF)
                parts += [hi, mid, low, bias]
            full = jnp.concatenate(parts, axis=0)
            for c in range(0, HID, 128):
                lh[slot, half, pr, c:c + 128, :] = full[:, c:c + 128].T

    def put_x(b, j, x):
        xb = x.astype(BF)
        pr, m = j // 2, j % 2
        for r in range(3):
            rx[b, pr, 64 * m + 16 * r:64 * m + 16 * r + 16, TOK * m:TOK * m + TOK] = xb

    def rx_prefix(b, s, c):
        for j in range(SB):
            put_x(b, j, s)
            s = s + fbuf[c, j]
        return s

    def body(cur, slot, half, finish, skip=False):
        def mm1(pr, lo):
            pre[1 - cur, pr, lo:lo + CW, :] = jnp.dot(lh[slot, half, pr, lo:lo + CW, :], rx[1 - cur, pr], preferred_element_type=F32)
        rows = []
        for pr in range(3):
            acc = jnp.zeros((16, 2 * TOK), F32)
            for lo in range(0, HID, CW):
                if not skip:
                    mm1(pr, lo)
                acc = acc + jnp.dot(w2[:, lo:lo + CW], act[1 - cur, pr, lo:lo + CW, :], preferred_element_type=F32)
                act[cur, pr, lo:lo + CW, :] = half_gelu(pre[cur, pr, lo:lo + CW, :]).astype(BF)
            rows += [acc[:, :TOK], acc[:, TOK:]]
        finish(rows)

    def tail(cur, finish):
        rows = []
        for pr in range(3):
            acc = jnp.dot(w2[...], act[cur, pr], preferred_element_type=F32)
            rows += [acc[:, :TOK], acc[:, TOK:]]
        finish(rows)

    def head(slot):
        for pr in range(3):
            for lo in range(0, HID, CW):
                pre[0, pr, lo:lo + CW, :] = jnp.dot(lh[slot, 0, pr, lo:lo + CW, :], rx[0, pr], preferred_element_type=F32)

    def store_f(c, kk, rows):
        tot = None
        for j in range(SB):
            f = hst[kk, j:j + 1, :] * rows[j]
            fbuf[c, j] = f
            tot = f if tot is None else tot + f
        return tot

    def wait_mods(k):
        pltpu.make_async_copy(gat.at[k], gat.at[k], gsem.at[k]).wait()
        pltpu.make_async_copy(hst.at[k], hst.at[k], hsem.at[k]).wait()

    def out_lh(g, half):
        return pltpu.make_async_copy(lh.at[g % 3, half], lhs_hbm.at[shift_chip(t, 2 * g + half, 1)], osem.at[g % 3, half])

    for g in range(2):
        for half in range(2):
            pltpu.make_async_copy(lh.at[g + 1, half], lhs_hbm.at[CHIPS + 2 * g + half], osem.at[g + 1, half]).start()
    for half in range(2):
        wait_mods(half)
        build(half, 0, half)
    for j in range(SB):
        put_x(0, j, x0[...])
        put_x(1, j, x0[...])
    head(0)

    def step0(i, more):
        for half in range(2):
            pltpu.make_async_copy(lh.at[(i + 1) % 3, half], lhs_hbm.at[half], osem.at[(i + 1) % 3, half]).wait()
            out_lh(i, half).start()
            if more:
                wait_mods(2 * i + 2 + half)
        for u in range(2):
            n = 2 * i + u
            if more:
                build(n + 2, (i + 1) % 3, u)
            prev = jnp.maximum(n - 1, 0)
            where = jnp.where(n == 0, CHIPS, shift_chip(t, prev, 1))
            body(u, (i + u) % 3, 1 - u, lambda rows: store_f(where, prev, rows), skip=(u == 1 and not more))

    def loop0(i, carry):
        step0(i, True)
        return carry

    lax.fori_loop(0, PAIRS - 1, loop0, 0)
    step0(PAIRS - 1, False)
    tail(1, lambda rows: store_f(shift_chip(t, CHIPS - 1, 1), CHIPS - 1, rows))
    for g in (PAIRS - 2, PAIRS - 1):
        for half in range(2):
            out_lh(g, half).wait()

    def block_of(s, n):
        if s < 3:
            return n
        return shift_chip(t, (n + 1) % CHIPS, 1)

    def in_lh(block, g, half):
        return pltpu.make_async_copy(lhs_hbm.at[block], lh.at[g % 3, half], lsem.at[g % 3, half])

    def send_f(k):
        c = shift_chip(t, k, 1)
        for pp in range(2):
            pltpu.make_async_remote_copy(fbuf.at[c, pl.ds(0, SB - 1)], r_out.at[:, row, :, pl.ds(col, TOK)],
                                         fsend.at[k], rsem, device_id=dev(c, pp), device_id_type=MESH).start()

    for g in range(2):
        for half in range(2):
            in_lh(2 * g + half, g, half).start()
    for half in range(2):
        in_lh(half, 0, half).wait()

    for s in (1, 2, 3):
        base = PAIRS * (s - 1)
        for b in range(2):
            if s < 3:
                run[0] = rx_prefix(b, run[0] if b else x0[...], b)
            else:
                rx_prefix(b, bas[block_of(3, b)], block_of(3, b))
            if b == 0:
                head(base % 3)

        def step(i, send, s=s, base=base):
            g = base + i
            for half in range(2):
                in_lh(0, g + 1, half).wait()
            for half in range(2):
                n = 2 * i + 4 + half
                nxt = block_of(min(s + 1, 3), n % CHIPS)
                in_lh(jnp.where(n < CHIPS, block_of(s, n % CHIPS), nxt), g + 2, half).start()
            if send:
                send_f(2 * i - 2)
                send_f(2 * i - 1)
            for u in range(2):
                n = 2 * i + u
                nx = jnp.minimum(n + 2, CHIPS - 1)
                prev = jnp.maximum(n - 1, 0)
                cp = block_of(s, prev)
                where = jnp.where(n == 0, CHIPS, cp)
                kk = shift_chip(cp, t, -1)

                def finish(rows):
                    tot = store_f(where, kk, rows)
                    if s == 2:
                        bas[where] = run[1]
                        run[1] = jnp.where(n == 0, x0[...], run[1] + tot)
                    if s == 3:
                        bas[where] = tot
                body(u, (g + u) % 3, 1 - u, finish)
                if s < 3:
                    run[0] = rx_prefix(u, run[0], nx)
                else:
                    cn = block_of(3, nx)
                    rx_prefix(u, bas[cn], cn)

        def loop(i, carry, step=step):
            step(i, False)
            return carry

        def loop_send(i, carry, step=step):
            step(i, True)
            return carry

        if s < 3:
            lax.fori_loop(0, PAIRS, loop, 0)
        else:
            lax.fori_loop(0, 2, loop, 0)
            send_f(1)
            lax.fori_loop(2, PAIRS, loop_send, 0)

        last = block_of(s, CHIPS - 1)

        def finish_last(rows, s=s, last=last):
            tot = store_f(last, shift_chip(last, t, -1) if s < 3 else 0, rows)
            if s == 2:
                bas[last] = run[1]
            if s == 3:
                bas[last] = tot
        tail(1, finish_last)

    send_f(CHIPS - 2)
    send_f(CHIPS - 1)
    for half in range(2):
        in_lh(0, 3 * PAIRS + 1, half).wait()
    own_f = pltpu.make_async_copy(fbuf.at[t, pl.ds(0, SB - 1)], r_out.at[:, row, :, pl.ds(col, TOK)], rsem)

    def scan_base(c, s):
        tot = bas[c]
        bas[c] = s
        return s + tot

    lax.fori_loop(0, CHIPS, scan_base, x0[...])

    def send_b(k, carry):
        c = shift_chip(t, k, 1)
        for pp in range(2):
            pltpu.make_async_remote_copy(bas.at[c], base_out.at[row, :, pl.ds(col, TOK)],
                                         bsend.at[k], bsem, device_id=dev(c, pp), device_id_type=MESH).start()
        return carry

    lax.fori_loop(1, CHIPS, send_b, 0)
    own_f.start()
    sib_f = pltpu.make_async_remote_copy(fbuf.at[t, pl.ds(0, SB - 1)], r_out.at[:, row, :, pl.ds(col, TOK)],
                                         fsib, rsem, device_id=dev(t, q), device_id_type=MESH)
    sib_f.start()
    pltpu.make_async_copy(bas.at[t], base_out.at[row, :, pl.ds(col, TOK)], bsem).start()
    sib_b = pltpu.make_async_remote_copy(bas.at[t], base_out.at[row, :, pl.ds(col, TOK)],
                                         bsib, bsem, device_id=dev(t, q), device_id_type=MESH)
    sib_b.start()

    cp_w.wait_send()
    cp_g0.wait_send()

    def drain(k, carry):
        pltpu.make_async_copy(gat.at[k], gat.at[k], gsend.at[k]).wait()
        pltpu.make_async_copy(hst.at[k], hst.at[k], hsend.at[k]).wait()
        pltpu.make_async_copy(fbuf.at[pl.ds(0, 2), pl.ds(0, SB - 1)], fbuf.at[pl.ds(0, 2), pl.ds(0, SB - 1)], fsend.at[k]).wait()
        pltpu.make_async_copy(bas.at[pl.ds(0, 2)], bas.at[pl.ds(0, 2)], bsend.at[k]).wait()
        return carry

    lax.fori_loop(1, CHIPS, drain, 0)
    sib_f.wait_send()
    sib_b.wait_send()
    pltpu.make_async_copy(r_out, r_out, rsem).wait()
    pltpu.make_async_copy(base_out, base_out, bsem).wait()


def sum_kernel(r_ref, b_ref, o_ref):
    s = b_ref[...]
    o_ref[0] = s
    for j in range(SB - 1):
        s = s + r_ref[j]
        o_ref[j + 1] = s


def solution(mesh):
    def device_body(x_init, w_up, w_down, mod_scale, mod_shift, step_size):
        batch, tokens, chan = x_init.shape
        p = lax.axis_index('model')

        def spread(a):
            tail = a[:, 512:]
            z = jnp.zeros_like(tail)
            last = jnp.where(p == 0, jnp.concatenate([tail, z], axis=1), jnp.concatenate([z, tail], axis=1))
            return jnp.concatenate([a[:, :512], last], axis=1)

        mods = spread(jnp.concatenate([mod_scale, mod_shift, jnp.zeros((4, mod_scale.shape[1]), BF)], axis=0))
        wts = spread(jnp.concatenate([w_up, w_down.T], axis=0))
        steps = jnp.broadcast_to(jnp.concatenate([step_size, jnp.zeros((2,), F32)])[:, None], (8, TOK))
        x0 = jnp.swapaxes(x_init, 1, 2)
        vm = pl.BlockSpec(memory_space=pltpu.VMEM)
        hb = pl.BlockSpec(memory_space=pl.ANY)
        dma = pltpu.SemaphoreType.DMA
        r, base, _ = pl.pallas_call(
            main_kernel,
            out_shape=(
                jax.ShapeDtypeStruct((SB - 1, batch, chan, tokens), F32),
                jax.ShapeDtypeStruct((batch, chan, tokens), F32),
                jax.ShapeDtypeStruct((CHIPS + 4, 3, HID, 128), BF),
            ),
            in_specs=[vm, vm, vm, hb],
            out_specs=(hb, hb, hb),
            scratch_shapes=[
                pltpu.VMEM((CHIPS, 2, 16, HALF), BF),
                pltpu.VMEM((CHIPS, 8, TOK), F32),
                pltpu.VMEM((2, 32, HALF), BF),
                pltpu.VMEM((chan, TOK), F32),
                pltpu.VMEM((chan, HID), F32),
                pltpu.VMEM((chan, HID), BF),
                pltpu.VMEM((3, 2, 3, HID, 128), BF),
                pltpu.VMEM((2, 3, 128, 2 * TOK), BF),
                pltpu.VMEM((2, 3, HID, 2 * TOK), F32),
                pltpu.VMEM((2, 3, HID, 2 * TOK), BF),
                pltpu.VMEM((CHIPS + 1, SB, chan, TOK), F32),
                pltpu.VMEM((CHIPS + 1, chan, TOK), F32),
                pltpu.VMEM((2, chan, TOK), F32),
                dma((CHIPS,)), dma((CHIPS,)), dma, dma((CHIPS,)), dma((CHIPS,)), dma, dma,
                dma((3, 2)), dma((3, 2)), dma((CHIPS,)), dma, dma((CHIPS,)), dma, dma, dma,
            ],
            compiler_params=pltpu.CompilerParams(has_side_effects=True, vmem_limit_bytes=60 * 2 ** 20),
            name='sweeps',
        )(mods, steps, wts, x0)
        tile = 1024
        out = pl.pallas_call(
            sum_kernel,
            grid=(batch, tokens // tile),
            out_shape=jax.ShapeDtypeStruct((SB, batch, chan, tokens), F32),
            in_specs=[pl.BlockSpec((SB - 1, None, chan, tile), lambda b, i: (0, b, 0, i)),
                      pl.BlockSpec((None, chan, tile), lambda b, i: (b, 0, i))],
            out_specs=pl.BlockSpec((SB, None, chan, tile), lambda b, i: (0, b, 0, i)),
            name='sums',
        )(r, base)
        return jnp.swapaxes(out, 2, 3)

    return jax.shard_map(device_body, mesh=mesh, in_specs=(P('data', None, None), P(None, 'model'), P('model', None), P('time', 'model'), P('time', 'model'), P('time')), out_specs=P('time', 'data', None, None), check_vma=False)
```

```python
import functools
import math

import jax
import jax.numpy as jnp
from jax import lax
from jax.experimental import pallas as pl
from jax.experimental.pallas import tpu as pltpu
from jax.sharding import PartitionSpec as P

MESH = pl.DeviceIdType.MESH
BF = jnp.bfloat16
F32 = jnp.float32
CHIPS = 64
SB = 6
HID = 1152
HALF = 640
TOK = 128
GC = math.sqrt(2.0 / math.pi)
G1 = 2.0 * GC
G2 = 8.0 * 0.044715 * GC
CW = 384
PAIRS = CHIPS // 2


def half_gelu(v):
    return v * jnp.tanh(v * (G1 + G2 * (v * v))) + v


def shift_chip(t, k, sign):
    out = 0
    for unit in (16, 4, 1):
        a = (t // unit) % 4
        b = (k // unit) % 4
        out = out + unit * ((a + sign * b + 4) % 4)
    return out


def main_kernel(scale, shift, up, down, hs, xmax, x0_hbm, r_out, base_out, lhs_hbm, flag,
                mods, steps, wts, gmax, gat, hst, wgt, x0, w1, w2, lh, rx, pre, act, fbuf, bas, run,
                gsem, hsem, wsem, gsend, hsend, wsend, xsem, osem, lsem, fsend, fsib, bsend, bsib, rsem, bsem):
    t = lax.axis_index('time')
    p = lax.axis_index('model')
    q = 1 - p
    blk = t * 2 + p
    row = blk // 32
    col = pl.multiple_of((blk % 32) * TOK, TOK)

    def dev(tt, pp):
        return {'time': tt, 'model': pp}

    cp_x = pltpu.make_async_copy(x0_hbm.at[row, :, pl.ds(col, TOK)], x0, xsem)
    cp_x.start()

    def spread(a):
        tail = a[:, 512:]
        z = jnp.zeros_like(tail)
        last = jnp.where(p == 0, jnp.concatenate([tail, z], axis=1), jnp.concatenate([z, tail], axis=1))
        return jnp.concatenate([a[:, :512], last], axis=1)

    mods[...] = spread(jnp.concatenate([scale[...].astype(F32), shift[...].astype(F32), jnp.zeros((4, scale.shape[1]), F32)], axis=0)).astype(BF)
    for j in range(SB):
        steps[j:j + 1, :] = jnp.full((1, TOK), hs[j], F32)
    steps[SB:8, :] = jnp.zeros((2, TOK), F32)
    wts[0:16, :] = spread(up[...].astype(F32)).astype(BF)
    wts[16:32, :] = spread(down[...].astype(F32)).astype(BF)
    gmax[...] = jnp.zeros(gmax.shape, F32)
    pltpu.make_async_copy(mods, gat.at[0, p], gsem.at[0]).start()
    pltpu.make_async_copy(steps, hst.at[0], hsem.at[0]).start()
    pltpu.make_async_copy(wts, wgt.at[p], wsem).start()
    cp_w = pltpu.make_async_remote_copy(wts, wgt.at[p], wsend, wsem, device_id=dev(t, q), device_id_type=MESH)
    cp_w.start()
    cp_g0 = pltpu.make_async_remote_copy(mods, gat.at[0, p], gsend.at[0], gsem.at[0], device_id=dev(t, q), device_id_type=MESH)
    cp_g0.start()

    def send_mods(k, carry):
        d = shift_chip(t, k, -1)
        for c in range(2):
            pltpu.make_async_remote_copy(mods, gat.at[k, p], gsend.at[k], gsem.at[k], device_id=dev(d, c), device_id_type=MESH).start()
        pltpu.make_async_remote_copy(steps, hst.at[k], hsend.at[k], hsem.at[k], device_id=dev(d, p), device_id_type=MESH).start()
        return carry

    lax.fori_loop(1, CHIPS, send_mods, 0)

    zero = jnp.zeros((16, TOK), BF)
    ones_row = jnp.where(lax.broadcasted_iota(jnp.int32, (16, TOK), 0) == 0, 1.0, 0.0).astype(BF)
    for b in range(2):
        for pr in range(3):
            for r in range(8):
                for m in range(2):
                    rx[b, pr, 16 * r:16 * r + 16, TOK * m:TOK * m + TOK] = ones_row if r == 4 * m + 3 else zero
    act[1] = jnp.zeros(act.shape[1:], BF)
    pltpu.make_async_copy(wgt, wgt, wsem).wait()
    wf = wgt[...].astype(F32)

    def merged(a, b):
        return jnp.concatenate([a[:, :512], b[:, :512], a[:, 512:] + b[:, 512:]], axis=1)

    w1[...] = merged(wf[0, :16], wf[1, :16])
    w2[...] = merged(wf[0, 16:], wf[1, 16:]).astype(BF)
    cp_x.wait()

    first = lax.broadcasted_iota(jnp.int32, (16, HID), 0) == 0

    def build(k, slot, half):
        mf = merged(gat[k, 0].astype(F32), gat[k, 1].astype(F32))
        w = w1[...]
        gmax[...] = jnp.maximum(gmax[...], jnp.abs(mf[:12]))
        for pr in range(3):
            parts = []
            for m in range(2):
                j = 2 * pr + m
                ws = w * (0.5 * mf[j:j + 1] + 0.5)
                hi = ws.astype(BF)
                rest = ws - hi.astype(F32)
                mid = rest.astype(BF)
                low = (rest - mid.astype(F32)).astype(BF)
                bias = jnp.where(first, 0.5 * mf[SB + j:SB + j + 1], 0.0).astype(BF)
                parts += [hi, mid, low, bias]
            full = jnp.concatenate(parts, axis=0)
            for c in range(0, HID, 128):
                lh[slot, half, pr, c:c + 128, :] = full[:, c:c + 128].T

    def put_x(b, j, x):
        xb = x.astype(BF)
        pr, m = j // 2, j % 2
        for r in range(3):
            rx[b, pr, 64 * m + 16 * r:64 * m + 16 * r + 16, TOK * m:TOK * m + TOK] = xb

    def rx_prefix(b, s, c):
        for j in range(SB):
            put_x(b, j, s)
            s = s + fbuf[c, j]
        return s

    def body(cur, slot, half, finish, skip=False):
        def mm1(pr, lo):
            pre[1 - cur, pr, lo:lo + CW, :] = jnp.dot(lh[slot, half, pr, lo:lo + CW, :], rx[1 - cur, pr], preferred_element_type=F32)
        rows = []
        for pr in range(3):
            acc = jnp.zeros((16, 2 * TOK), F32)
            for lo in range(0, HID, CW):
                if not skip:
                    mm1(pr, lo)
                acc = acc + jnp.dot(w2[:, lo:lo + CW], act[1 - cur, pr, lo:lo + CW, :], preferred_element_type=F32)
                act[cur, pr, lo:lo + CW, :] = half_gelu(pre[cur, pr, lo:lo + CW, :]).astype(BF)
            rows += [acc[:, :TOK], acc[:, TOK:]]
        finish(rows)

    def tail(cur, finish):
        rows = []
        for pr in range(3):
            acc = jnp.dot(w2[...], act[cur, pr], preferred_element_type=F32)
            rows += [acc[:, :TOK], acc[:, TOK:]]
        finish(rows)

    def head(slot):
        for pr in range(3):
            for lo in range(0, HID, CW):
                pre[0, pr, lo:lo + CW, :] = jnp.dot(lh[slot, 0, pr, lo:lo + CW, :], rx[0, pr], preferred_element_type=F32)

    def store_f(c, kk, rows):
        tot = None
        for j in range(SB):
            f = hst[kk, j:j + 1, :] * rows[j]
            fbuf[c, j] = f
            tot = f if tot is None else tot + f
        return tot

    def wait_mods(k):
        pltpu.make_async_copy(gat.at[k], gat.at[k], gsem.at[k]).wait()
        pltpu.make_async_copy(hst.at[k], hst.at[k], hsem.at[k]).wait()

    def out_lh(g, half):
        return pltpu.make_async_copy(lh.at[g % 3, half], lhs_hbm.at[shift_chip(t, 2 * g + half, 1)], osem.at[g % 3, half])

    for g in range(2):
        for half in range(2):
            pltpu.make_async_copy(lh.at[g + 1, half], lhs_hbm.at[CHIPS + 2 * g + half], osem.at[g + 1, half]).start()
    for half in range(2):
        wait_mods(half)
        build(half, 0, half)
    for j in range(SB):
        put_x(0, j, x0[...])
        put_x(1, j, x0[...])
    head(0)

    def step0(i, more):
        for half in range(2):
            pltpu.make_async_copy(lh.at[(i + 1) % 3, half], lhs_hbm.at[half], osem.at[(i + 1) % 3, half]).wait()
            out_lh(i, half).start()
            if more:
                wait_mods(2 * i + 2 + half)
        for u in range(2):
            n = 2 * i + u
            if more:
                build(n + 2, (i + 1) % 3, u)
            prev = jnp.maximum(n - 1, 0)
            where = jnp.where(n == 0, CHIPS, shift_chip(t, prev, 1))
            body(u, (i + u) % 3, 1 - u, lambda rows: store_f(where, prev, rows), skip=(u == 1 and not more))

    def loop0(i, carry):
        step0(i, True)
        return carry

    lax.fori_loop(0, PAIRS - 1, loop0, 0)
    step0(PAIRS - 1, False)
    tail(1, lambda rows: store_f(shift_chip(t, CHIPS - 1, 1), CHIPS - 1, rows))
    for g in (PAIRS - 2, PAIRS - 1):
        for half in range(2):
            out_lh(g, half).wait()

    def top(a):
        return jnp.max(jnp.max(a, axis=1, keepdims=True), axis=0, keepdims=True)

    wa = jnp.abs(w1[...])
    wtop = top(wa)
    wlow = -top(-jnp.where(wa == 0.0, 1.0, wa))
    gtop = 1.0 + top(gmax[0:SB])
    btop = top(gmax[SB:2 * SB])
    dtop = top(jnp.abs(w2[...].astype(F32)))
    habs = lax.fori_loop(0, CHIPS, lambda k, a: a + jnp.abs(hst[k]), jnp.zeros((8, TOK), F32))
    hsum = 8.0 * top(habs)
    xtop = jnp.full((1, 1), xmax[0], F32)
    bound = xtop
    for _ in range(4):
        arg = 16.0 * bound * (1.0 + wtop) * gtop + btop
        bound = xtop + hsum * (HID * 2.0) * dtop * arg
    safe = (16.0 * bound * (1.0 + wtop) * gtop < 2.0 ** 100) & (wlow > 2.0 ** -80)
    flag[...] = jnp.broadcast_to(jnp.where(safe, 1.0, 0.0), (8, TOK))

    def block_of(s, n):
        if s < 3:
            return n
        return shift_chip(t, (n + 1) % CHIPS, 1)

    def in_lh(block, g, half):
        return pltpu.make_async_copy(lhs_hbm.at[block], lh.at[g % 3, half], lsem.at[g % 3, half])

    def send_f(k):
        c = shift_chip(t, k, 1)
        for pp in range(2):
            pltpu.make_async_remote_copy(fbuf.at[c, pl.ds(0, SB - 1)], r_out.at[:, row, :, pl.ds(col, TOK)],
                                         fsend.at[k], rsem, device_id=dev(c, pp), device_id_type=MESH).start()

    for g in range(2):
        for half in range(2):
            in_lh(2 * g + half, g, half).start()
    for half in range(2):
        in_lh(half, 0, half).wait()

    for s in (1, 2, 3):
        base = PAIRS * (s - 1)
        for b in range(2):
            if s < 3:
                run[0] = rx_prefix(b, run[0] if b else x0[...], b)
            else:
                rx_prefix(b, bas[block_of(3, b)], block_of(3, b))
            if b == 0:
                head(base % 3)

        def step(i, send, s=s, base=base):
            g = base + i
            for half in range(2):
                in_lh(0, g + 1, half).wait()
            for half in range(2):
                n = 2 * i + 4 + half
                nxt = block_of(min(s + 1, 3), n % CHIPS)
                in_lh(jnp.where(n < CHIPS, block_of(s, n % CHIPS), nxt), g + 2, half).start()
            if send:
                send_f(2 * i - 2)
                send_f(2 * i - 1)
            for u in range(2):
                n = 2 * i + u
                nx = jnp.minimum(n + 2, CHIPS - 1)
                prev = jnp.maximum(n - 1, 0)
                cp = block_of(s, prev)
                where = jnp.where(n == 0, CHIPS, cp)
                kk = shift_chip(cp, t, -1)

                def finish(rows):
                    tot = store_f(where, kk, rows)
                    if s == 2:
                        bas[where] = run[1]
                        run[1] = jnp.where(n == 0, x0[...], run[1] + tot)
                    if s == 3:
                        bas[where] = tot
                body(u, (g + u) % 3, 1 - u, finish)
                if s < 3:
                    run[0] = rx_prefix(u, run[0], nx)
                else:
                    cn = block_of(3, nx)
                    rx_prefix(u, bas[cn], cn)

        def loop(i, carry, step=step):
            step(i, False)
            return carry

        def loop_send(i, carry, step=step):
            step(i, True)
            return carry

        if s < 3:
            lax.fori_loop(0, PAIRS, loop, 0)
        else:
            lax.fori_loop(0, 2, loop, 0)
            send_f(1)
            lax.fori_loop(2, PAIRS, loop_send, 0)

        last = block_of(s, CHIPS - 1)

        def finish_last(rows, s=s, last=last):
            tot = store_f(last, shift_chip(last, t, -1) if s < 3 else 0, rows)
            if s == 2:
                bas[last] = run[1]
            if s == 3:
                bas[last] = tot
        tail(1, finish_last)

    send_f(CHIPS - 2)
    send_f(CHIPS - 1)
    for half in range(2):
        in_lh(0, 3 * PAIRS + 1, half).wait()
    own_f = pltpu.make_async_copy(fbuf.at[t, pl.ds(0, SB - 1)], r_out.at[:, row, :, pl.ds(col, TOK)], rsem)

    def scan_base(c, s):
        tot = bas[c]
        bas[c] = s
        return s + tot

    lax.fori_loop(0, CHIPS, scan_base, x0[...])

    def send_b(k, carry):
        c = shift_chip(t, k, 1)
        for pp in range(2):
            pltpu.make_async_remote_copy(bas.at[c], base_out.at[row, :, pl.ds(col, TOK)],
                                         bsend.at[k], bsem, device_id=dev(c, pp), device_id_type=MESH).start()
        return carry

    lax.fori_loop(1, CHIPS, send_b, 0)
    own_f.start()
    sib_f = pltpu.make_async_remote_copy(fbuf.at[t, pl.ds(0, SB - 1)], r_out.at[:, row, :, pl.ds(col, TOK)],
                                         fsib, rsem, device_id=dev(t, q), device_id_type=MESH)
    sib_f.start()
    pltpu.make_async_copy(bas.at[t], base_out.at[row, :, pl.ds(col, TOK)], bsem).start()
    sib_b = pltpu.make_async_remote_copy(bas.at[t], base_out.at[row, :, pl.ds(col, TOK)],
                                         bsib, bsem, device_id=dev(t, q), device_id_type=MESH)
    sib_b.start()

    cp_w.wait_send()
    cp_g0.wait_send()

    def drain(k, carry):
        pltpu.make_async_copy(gat.at[k], gat.at[k], gsend.at[k]).wait()
        pltpu.make_async_copy(hst.at[k], hst.at[k], hsend.at[k]).wait()
        pltpu.make_async_copy(fbuf.at[pl.ds(0, 2), pl.ds(0, SB - 1)], fbuf.at[pl.ds(0, 2), pl.ds(0, SB - 1)], fsend.at[k]).wait()
        pltpu.make_async_copy(bas.at[pl.ds(0, 2)], bas.at[pl.ds(0, 2)], bsend.at[k]).wait()
        return carry

    lax.fori_loop(1, CHIPS, drain, 0)
    sib_f.wait_send()
    sib_b.wait_send()
    pltpu.make_async_copy(r_out, r_out, rsem).wait()
    pltpu.make_async_copy(base_out, base_out, bsem).wait()


def sum_kernel(r_ref, b_ref, o_ref):
    s = b_ref[...]
    o_ref[0] = s
    for j in range(SB - 1):
        s = s + r_ref[j]
        o_ref[j + 1] = s


def plain(x_init, w_up, w_down, mod_scale, mod_shift, step_size):
    time_devs = lax.axis_size('time')
    scale_f = 1.0 + mod_scale.astype(F32)
    shift_f = mod_shift.astype(F32)
    step_col = step_size[:, None, None, None]

    def drift(args):
        lat, sc, sh = args
        act = jnp.einsum('bnc,cd->bnd', lat.astype(BF), w_up, preferred_element_type=F32)
        hidden = jax.nn.gelu(act * sc + sh, approximate=True)
        return jnp.einsum('bnd,dc->bnc', hidden.astype(BF), w_down, preferred_element_type=F32)

    def sweep(_, latents):
        part = lax.map(drift, (latents, scale_f, shift_f))
        drifts = step_col * (part + lax.ppermute(part, 'model', [(0, 1), (1, 0)]))
        running = jnp.cumsum(drifts, axis=0)
        total = running[-1]
        acc = total
        hop = 1
        while hop < time_devs:
            acc = acc + lax.ppermute(acc, 'time', [(a, a + hop) for a in range(time_devs - hop)])
            hop = hop * 2
        return (x_init + (acc - total))[None] + (running - drifts)

    start = jnp.broadcast_to(x_init[None], (mod_scale.shape[0],) + x_init.shape)
    return lax.fori_loop(0, 4, sweep, start)


def solution(mesh):
    def device_body(x_init, w_up, w_down, mod_scale, mod_shift, step_size):
        batch, tokens, chan = x_init.shape
        x0 = jnp.swapaxes(x_init, 1, 2)
        xmax = jnp.max(jnp.abs(x_init)).reshape(1)
        vm = pl.BlockSpec(memory_space=pltpu.VMEM)
        sm = pl.BlockSpec(memory_space=pltpu.SMEM)
        hb = pl.BlockSpec(memory_space=pl.ANY)
        dma = pltpu.SemaphoreType.DMA
        r, base, _, flag = pl.pallas_call(
            main_kernel,
            out_shape=(
                jax.ShapeDtypeStruct((SB - 1, batch, chan, tokens), F32),
                jax.ShapeDtypeStruct((batch, chan, tokens), F32),
                jax.ShapeDtypeStruct((CHIPS + 4, 3, HID, 128), BF),
                jax.ShapeDtypeStruct((8, TOK), F32),
            ),
            in_specs=[vm, vm, vm, vm, sm, sm, hb],
            out_specs=(hb, hb, hb, vm),
            scratch_shapes=[
                pltpu.VMEM((16, HALF), BF),
                pltpu.VMEM((8, TOK), F32),
                pltpu.VMEM((32, HALF), BF),
                pltpu.VMEM((2 * SB, HID), F32),
                pltpu.VMEM((CHIPS, 2, 16, HALF), BF),
                pltpu.VMEM((CHIPS, 8, TOK), F32),
                pltpu.VMEM((2, 32, HALF), BF),
                pltpu.VMEM((chan, TOK), F32),
                pltpu.VMEM((chan, HID), F32),
                pltpu.VMEM((chan, HID), BF),
                pltpu.VMEM((3, 2, 3, HID, 128), BF),
                pltpu.VMEM((2, 3, 128, 2 * TOK), BF),
                pltpu.VMEM((2, 3, HID, 2 * TOK), F32),
                pltpu.VMEM((2, 3, HID, 2 * TOK), BF),
                pltpu.VMEM((CHIPS + 1, SB, chan, TOK), F32),
                pltpu.VMEM((CHIPS + 1, chan, TOK), F32),
                pltpu.VMEM((2, chan, TOK), F32),
                dma((CHIPS,)), dma((CHIPS,)), dma, dma((CHIPS,)), dma((CHIPS,)), dma, dma,
                dma((3, 2)), dma((3, 2)), dma((CHIPS,)), dma, dma((CHIPS,)), dma, dma, dma,
            ],
            compiler_params=pltpu.CompilerParams(has_side_effects=True, vmem_limit_bytes=60 * 2 ** 20),
            name='sweeps',
        )(mod_scale, mod_shift, w_up, w_down.T, step_size, xmax, x0)
        tile = 2048

        def fast():
            out = pl.pallas_call(
                sum_kernel,
                grid=(batch, tokens // tile),
                out_shape=jax.ShapeDtypeStruct((SB, batch, chan, tokens), F32),
                in_specs=[pl.BlockSpec((SB - 1, None, chan, tile), lambda b, i: (0, b, 0, i)),
                          pl.BlockSpec((None, chan, tile), lambda b, i: (b, 0, i))],
                out_specs=pl.BlockSpec((SB, None, chan, tile), lambda b, i: (0, b, 0, i)),
                name='sums',
            )(r, base)
            return jnp.swapaxes(out, 2, 3)

        def slow():
            return plain(x_init, w_up, w_down, mod_scale, mod_shift, step_size)

        return lax.cond(flag[0, 0] > 0.5, fast, slow)

    return jax.shard_map(device_body, mesh=mesh, in_specs=(P('data', None, None), P(None, 'model'), P('model', None), P('time', 'model'), P('time', 'model'), P('time')), out_specs=P('time', 'data', None, None), check_vma=False)
```

```python
import functools
import math

import jax
import jax.numpy as jnp
from jax import lax
from jax.experimental import pallas as pl
from jax.experimental.pallas import tpu as pltpu
from jax.sharding import PartitionSpec as P

MESH = pl.DeviceIdType.MESH
BF = jnp.bfloat16
F32 = jnp.float32
CHIPS = 64
SB = 6
HID = 1152
HALF = 640
TOK = 128
GC = math.sqrt(2.0 / math.pi)
G1 = 2.0 * GC
G2 = 8.0 * 0.044715 * GC
CW = 384
PAIRS = CHIPS // 2


def half_gelu(v):
    return v * jnp.tanh(v * (G1 + G2 * (v * v))) + v


def shift_chip(t, k, sign):
    out = 0
    for unit in (16, 4, 1):
        a = lax.rem(lax.div(jnp.int32(t), jnp.int32(unit)), jnp.int32(4))
        b = lax.rem(lax.div(jnp.int32(k), jnp.int32(unit)), jnp.int32(4))
        out = out + unit * lax.rem(a + sign * b + 4, jnp.int32(4))
    return out


def main_kernel(scale, shift, up, down, hs, x0_hbm, r_out, base_out, lhs_hbm, flag,
                mods, steps, wts, gmax, gat, hst, wgt, x0, w1, w2, lh, rx, pre, act, fbuf, bas, run,
                gsem, hsem, wsem, gsend, hsend, wsend, xsem, osem, lsem, fsend, psend, bsend, bsib, rsem, psem, bsem, bpsem, xall, xallsem):
    t = lax.axis_index('time')
    p = lax.axis_index('model')
    q = 1 - p
    row = 2 * p + lax.div(t, jnp.int32(32))
    col = pl.multiple_of(lax.rem(t, jnp.int32(32)) * TOK, TOK)

    def dev(tt, pp):
        return {'time': tt, 'model': pp}

    cp_x = pltpu.make_async_copy(x0_hbm.at[row, :, pl.ds(col, TOK)], x0, xsem)
    cp_x.start()
    cp_all = pltpu.make_async_copy(x0_hbm, xall, xallsem)
    cp_all.start()

    def spread(a):
        tail = a[:, 512:]
        z = jnp.zeros_like(tail)
        last = jnp.where(p == 0, jnp.concatenate([tail, z], axis=1), jnp.concatenate([z, tail], axis=1))
        return jnp.concatenate([a[:, :512], last], axis=1)

    mods[...] = spread(jnp.concatenate([scale[...].astype(F32), shift[...].astype(F32), jnp.zeros((4, scale.shape[1]), F32)], axis=0)).astype(BF)
    for j in range(SB):
        steps[j:j + 1, :] = jnp.full((1, TOK), hs[j], F32)
    steps[SB:8, :] = jnp.zeros((2, TOK), F32)
    wts[0:16, :] = spread(up[...].astype(F32)).astype(BF)
    wts[16:32, :] = spread(down[...].astype(F32)).astype(BF)
    gmax[...] = jnp.zeros(gmax.shape, F32)
    pltpu.make_async_copy(mods, gat.at[0, p], gsem.at[0]).start()
    pltpu.make_async_copy(steps, hst.at[0], hsem.at[0]).start()
    pltpu.make_async_copy(wts, wgt.at[p], wsem).start()
    cp_w = pltpu.make_async_remote_copy(wts, wgt.at[p], wsend, wsem, device_id=dev(t, q), device_id_type=MESH)
    cp_w.start()
    cp_g0 = pltpu.make_async_remote_copy(mods, gat.at[0, p], gsend.at[0], gsem.at[0], device_id=dev(t, q), device_id_type=MESH)
    cp_g0.start()

    def send_mods(k, carry):
        d = shift_chip(t, k, -1)
        for c in range(2):
            pltpu.make_async_remote_copy(mods, gat.at[k, p], gsend.at[k], gsem.at[k], device_id=dev(d, c), device_id_type=MESH).start()
        pltpu.make_async_remote_copy(steps, hst.at[k], hsend.at[k], hsem.at[k], device_id=dev(d, p), device_id_type=MESH).start()
        return carry

    lax.fori_loop(1, CHIPS, send_mods, 0)

    zero = jnp.zeros((16, TOK), BF)
    ones_row = jnp.where(lax.broadcasted_iota(jnp.int32, (16, TOK), 0) == 0, 1.0, 0.0).astype(BF)
    for b in range(2):
        for pr in range(3):
            for r in range(8):
                for m in range(2):
                    rx[b, pr, 16 * r:16 * r + 16, TOK * m:TOK * m + TOK] = ones_row if r == 4 * m + 3 else zero
    act[1] = jnp.zeros(act.shape[1:], BF)
    pltpu.make_async_copy(wgt, wgt, wsem).wait()
    wf = wgt[...].astype(F32)

    def merged(a, b):
        return jnp.concatenate([a[:, :512], b[:, :512], a[:, 512:] + b[:, 512:]], axis=1)

    w1[...] = merged(wf[0, :16], wf[1, :16])
    w2[...] = merged(wf[0, 16:], wf[1, 16:]).astype(BF)
    cp_x.wait()

    first = lax.broadcasted_iota(jnp.int32, (16, HID), 0) == 0

    def build(k, slot, half):
        mf = merged(gat[k, 0].astype(F32), gat[k, 1].astype(F32))
        w = w1[...]
        gmax[...] = jnp.maximum(gmax[...], jnp.abs(mf[:12]))
        for pr in range(3):
            parts = []
            for m in range(2):
                j = 2 * pr + m
                ws = w * (0.5 * mf[j:j + 1] + 0.5)
                hi = ws.astype(BF)
                rest = ws - hi.astype(F32)
                mid = rest.astype(BF)
                low = (rest - mid.astype(F32)).astype(BF)
                bias = jnp.where(first, 0.5 * mf[SB + j:SB + j + 1], 0.0).astype(BF)
                parts += [hi, mid, low, bias]
            full = jnp.concatenate(parts, axis=0)
            for c in range(0, HID, 128):
                lh[slot, half, pr, c:c + 128, :] = full[:, c:c + 128].T

    def put_x(b, j, x):
        xb = x.astype(BF)
        pr, m = j // 2, j % 2
        for r in range(3):
            rx[b, pr, 64 * m + 16 * r:64 * m + 16 * r + 16, TOK * m:TOK * m + TOK] = xb

    def rx_prefix(b, s, c):
        for j in range(SB):
            put_x(b, j, s)
            s = s + fbuf[c, j]
        return s

    def body(cur, slot, half, finish, skip=False):
        def mm1(pr, lo):
            pre[1 - cur, pr, lo:lo + CW, :] = jnp.dot(lh[slot, half, pr, lo:lo + CW, :], rx[1 - cur, pr], preferred_element_type=F32)
        rows = []
        for pr in range(3):
            acc = jnp.zeros((16, 2 * TOK), F32)
            for lo in range(0, HID, CW):
                if not skip:
                    mm1(pr, lo)
                acc = acc + jnp.dot(w2[:, lo:lo + CW], act[1 - cur, pr, lo:lo + CW, :], preferred_element_type=F32)
                act[cur, pr, lo:lo + CW, :] = half_gelu(pre[cur, pr, lo:lo + CW, :]).astype(BF)
            rows += [acc[:, :TOK], acc[:, TOK:]]
        finish(rows)

    def tail(cur, finish):
        rows = []
        for pr in range(3):
            acc = jnp.dot(w2[...], act[cur, pr], preferred_element_type=F32)
            rows += [acc[:, :TOK], acc[:, TOK:]]
        finish(rows)

    def head(slot):
        for pr in range(3):
            for lo in range(0, HID, CW):
                pre[0, pr, lo:lo + CW, :] = jnp.dot(lh[slot, 0, pr, lo:lo + CW, :], rx[0, pr], preferred_element_type=F32)

    def store_f(c, kk, rows):
        tot = None
        for j in range(SB):
            f = hst[kk, j:j + 1, :] * rows[j]
            fbuf[c, j] = f
            tot = f if tot is None else tot + f
        return tot

    def wait_mods(k):
        pltpu.make_async_copy(gat.at[k], gat.at[k], gsem.at[k]).wait()
        pltpu.make_async_copy(hst.at[k], hst.at[k], hsem.at[k]).wait()

    def out_lh(g, half):
        return pltpu.make_async_copy(lh.at[g % 3, half], lhs_hbm.at[shift_chip(t, 2 * g + half, 1)], osem.at[g % 3, half])

    for g in range(2):
        for half in range(2):
            pltpu.make_async_copy(lh.at[g + 1, half], lhs_hbm.at[CHIPS + 2 * g + half], osem.at[g + 1, half]).start()
    for half in range(2):
        wait_mods(half)
        build(half, 0, half)
    for j in range(SB):
        put_x(0, j, x0[...])
        put_x(1, j, x0[...])
    head(0)

    def step0(i, more):
        for half in range(2):
            pltpu.make_async_copy(lh.at[(i + 1) % 3, half], lhs_hbm.at[half], osem.at[(i + 1) % 3, half]).wait()
            out_lh(i, half).start()
            if more:
                wait_mods(2 * i + 2 + half)
        for u in range(2):
            n = 2 * i + u
            if more:
                build(n + 2, (i + 1) % 3, u)
            prev = jnp.maximum(n - 1, 0)
            where = jnp.where(n == 0, CHIPS, shift_chip(t, prev, 1))
            body(u, (i + u) % 3, 1 - u, lambda rows: store_f(where, prev, rows), skip=(u == 1 and not more))

    def loop0(i, carry):
        step0(i, True)
        return carry

    lax.fori_loop(0, PAIRS - 1, loop0, 0)
    step0(PAIRS - 1, False)
    tail(1, lambda rows: store_f(shift_chip(t, CHIPS - 1, 1), CHIPS - 1, rows))
    for g in (PAIRS - 2, PAIRS - 1):
        for half in range(2):
            out_lh(g, half).wait()

    def top(a):
        return jnp.max(jnp.max(a, axis=1, keepdims=True), axis=0, keepdims=True)

    wa = jnp.abs(w1[...])
    wtop = top(wa)
    wlow = -top(-jnp.where(wa == 0.0, 1.0, wa))
    gtop = 1.0 + top(gmax[0:SB])
    btop = top(gmax[SB:2 * SB])
    dtop = top(jnp.abs(w2[...].astype(F32)))
    habs = lax.fori_loop(0, CHIPS, lambda k, a: a + jnp.abs(hst[k]), jnp.zeros((8, TOK), F32))
    hsum = 8.0 * top(habs)
    cp_all.wait()
    xtop = top(jnp.max(jnp.abs(xall[...]), axis=0))
    bound = xtop
    for _ in range(4):
        arg = 16.0 * bound * (1.0 + wtop) * gtop + btop
        bound = xtop + hsum * (HID * 2.0) * dtop * arg
    safe = (16.0 * bound * (1.0 + wtop) * gtop < 2.0 ** 100) & (wlow > 2.0 ** -80)
    flag[...] = jnp.broadcast_to(jnp.where(safe, 1.0, 0.0), (8, TOK))

    def block_of(s, n):
        if s < 3:
            return n
        return shift_chip(t, lax.rem(jnp.int32(n + 1), jnp.int32(CHIPS)), 1)

    def in_lh(block, g, half):
        return pltpu.make_async_copy(lhs_hbm.at[block], lh.at[g % 3, half], lsem.at[g % 3, half])

    def send_f(k):
        c = shift_chip(t, k, 1)
        pltpu.make_async_remote_copy(fbuf.at[c, pl.ds(0, SB - 1)], r_out.at[:, row, :, pl.ds(col, TOK)],
                                     fsend.at[k], rsem.at[k], device_id=dev(c, p), device_id_type=MESH).start()

    def pass_on(k):
        src = shift_chip(t, k, -1)
        part = r_out.at[:, 2 * p + lax.div(src, jnp.int32(32)), :, pl.ds(pl.multiple_of(lax.rem(src, jnp.int32(32)) * TOK, TOK), TOK)]
        pltpu.make_async_copy(part, part, rsem.at[k]).wait()
        pltpu.make_async_remote_copy(part, part, psend.at[k], psem, device_id=dev(t, q), device_id_type=MESH).start()

    for g in range(2):
        for half in range(2):
            in_lh(2 * g + half, g, half).start()
    for half in range(2):
        in_lh(half, 0, half).wait()

    for s in (1, 2, 3):
        base = PAIRS * (s - 1)
        for b in range(2):
            if s < 3:
                run[0] = rx_prefix(b, run[0] if b else x0[...], b)
            else:
                rx_prefix(b, bas[block_of(3, b)], block_of(3, b))
            if b == 0:
                head(base % 3)

        def step(i, send, s=s, base=base):
            g = base + i
            for half in range(2):
                in_lh(0, g + 1, half).wait()
            for half in range(2):
                n = 2 * i + 4 + half
                wrap = lax.rem(n, jnp.int32(CHIPS))
                nxt = block_of(min(s + 1, 3), wrap)
                in_lh(jnp.where(n < CHIPS, block_of(s, wrap), nxt), g + 2, half).start()
            if send:
                send_f(2 * i - 2)
                send_f(2 * i - 1)
                pass_on(2 * i - 7)
                pass_on(2 * i - 6)
            for u in range(2):
                n = 2 * i + u
                nx = jnp.minimum(n + 2, CHIPS - 1)
                prev = jnp.maximum(n - 1, 0)
                cp = block_of(s, prev)
                where = jnp.where(n == 0, CHIPS, cp)
                kk = shift_chip(cp, t, -1)

                def finish(rows):
                    tot = store_f(where, kk, rows)
                    if s == 2:
                        bas[where] = run[1]
                        run[1] = jnp.where(n == 0, x0[...], run[1] + tot)
                    if s == 3:
                        bas[where] = tot
                body(u, (g + u) % 3, 1 - u, finish)
                if s < 3:
                    run[0] = rx_prefix(u, run[0], nx)
                else:
                    cn = block_of(3, nx)
                    rx_prefix(u, bas[cn], cn)

        def loop(i, carry, step=step):
            step(i, False)
            return carry

        def loop_send(i, carry, step=step):
            step(i, True)
            return carry

        if s < 3:
            lax.fori_loop(0, PAIRS, loop, 0)
        else:
            lax.fori_loop(0, 4, loop, 0)
            for k in range(1, 6):
                send_f(k)
            lax.fori_loop(4, PAIRS, loop_send, 0)

        last = block_of(s, CHIPS - 1)

        def finish_last(rows, s=s, last=last):
            tot = store_f(last, shift_chip(last, t, -1) if s < 3 else 0, rows)
            if s == 2:
                bas[last] = run[1]
            if s == 3:
                bas[last] = tot
        tail(1, finish_last)

    send_f(CHIPS - 2)
    send_f(CHIPS - 1)
    for half in range(2):
        in_lh(0, 3 * PAIRS + 1, half).wait()
    mine = r_out.at[:, row, :, pl.ds(col, TOK)]
    own_f = pltpu.make_async_copy(fbuf.at[t, pl.ds(0, SB - 1)], mine, rsem.at[0])
    own_f.start()
    sib_f = pltpu.make_async_remote_copy(fbuf.at[t, pl.ds(0, SB - 1)], mine, psend.at[0], psem, device_id=dev(t, q), device_id_type=MESH)
    sib_f.start()

    def scan_base(c, s):
        tot = bas[c]
        bas[c] = s
        return s + tot

    lax.fori_loop(0, CHIPS, scan_base, x0[...])

    def send_b(k, carry):
        c = shift_chip(t, k, 1)
        pltpu.make_async_remote_copy(bas.at[c], base_out.at[row, :, pl.ds(col, TOK)],
                                     bsend.at[k], bsem, device_id=dev(c, p), device_id_type=MESH).start()
        return carry

    lax.fori_loop(1, CHIPS, send_b, 0)
    pltpu.make_async_copy(bas.at[t], base_out.at[row, :, pl.ds(col, TOK)], bsem).start()

    def late(k, carry):
        pass_on(k)
        return carry

    lax.fori_loop(CHIPS - 7, CHIPS, late, 0)
    half_b = base_out.at[pl.ds(2 * p, 2)]
    pltpu.make_async_copy(half_b, half_b, bsem).wait()
    sib_b = pltpu.make_async_remote_copy(half_b, half_b, bsib, bpsem, device_id=dev(t, q), device_id_type=MESH)
    sib_b.start()

    cp_w.wait_send()
    cp_g0.wait_send()

    def drain(k, carry):
        pltpu.make_async_copy(gat.at[k], gat.at[k], gsend.at[k]).wait()
        pltpu.make_async_copy(hst.at[k], hst.at[k], hsend.at[k]).wait()
        pltpu.make_async_copy(fbuf.at[k, pl.ds(0, SB - 1)], fbuf.at[k, pl.ds(0, SB - 1)], fsend.at[k]).wait()
        pltpu.make_async_copy(fbuf.at[k, pl.ds(0, SB - 1)], fbuf.at[k, pl.ds(0, SB - 1)], psend.at[k]).wait()
        pltpu.make_async_copy(bas.at[k], bas.at[k], bsend.at[k]).wait()
        return carry

    lax.fori_loop(1, CHIPS, drain, 0)
    sib_f.wait_send()
    sib_b.wait_send()
    own_f.wait()
    theirs = r_out.at[:, pl.ds(2 * q, 2)]
    pltpu.make_async_copy(theirs, theirs, psem).wait()
    half_q = base_out.at[pl.ds(2 * q, 2)]
    pltpu.make_async_copy(half_q, half_q, bpsem).wait()


def sum_kernel(r_ref, b_ref, o_ref):
    s = b_ref[...]
    o_ref[0] = s
    for j in range(SB - 1):
        s = s + r_ref[j]
        o_ref[j + 1] = s


def plain(x_init, w_up, w_down, mod_scale, mod_shift, step_size):
    time_devs = lax.axis_size('time')
    scale_f = 1.0 + mod_scale.astype(F32)
    shift_f = mod_shift.astype(F32)
    step_col = step_size[:, None, None, None]

    def drift(args):
        lat, sc, sh = args
        act = jnp.einsum('bnc,cd->bnd', lat.astype(BF), w_up, preferred_element_type=F32)
        hidden = jax.nn.gelu(act * sc + sh, approximate=True)
        return jnp.einsum('bnd,dc->bnc', hidden.astype(BF), w_down, preferred_element_type=F32)

    def sweep(_, latents):
        part = lax.map(drift, (latents, scale_f, shift_f))
        drifts = step_col * (part + lax.ppermute(part, 'model', [(0, 1), (1, 0)]))
        running = jnp.cumsum(drifts, axis=0)
        total = running[-1]
        acc = total
        hop = 1
        while hop < time_devs:
            acc = acc + lax.ppermute(acc, 'time', [(a, a + hop) for a in range(time_devs - hop)])
            hop = hop * 2
        return (x_init + (acc - total))[None] + (running - drifts)

    start = jnp.broadcast_to(x_init[None], (mod_scale.shape[0],) + x_init.shape)
    return lax.fori_loop(0, 4, sweep, start)


def solution(mesh):
    def device_body(x_init, w_up, w_down, mod_scale, mod_shift, step_size):
        batch, tokens, chan = x_init.shape
        x0 = jnp.swapaxes(x_init, 1, 2)
        vm = pl.BlockSpec(memory_space=pltpu.VMEM)
        sm = pl.BlockSpec(memory_space=pltpu.SMEM)
        hb = pl.BlockSpec(memory_space=pl.ANY)
        dma = pltpu.SemaphoreType.DMA
        r, base, _, flag = pl.pallas_call(
            main_kernel,
            out_shape=(
                jax.ShapeDtypeStruct((SB - 1, batch, chan, tokens), F32),
                jax.ShapeDtypeStruct((batch, chan, tokens), F32),
                jax.ShapeDtypeStruct((CHIPS + 4, 3, HID, 128), BF),
                jax.ShapeDtypeStruct((8, TOK), F32),
            ),
            in_specs=[vm, vm, vm, vm, sm, hb],
            out_specs=(hb, hb, hb, vm),
            scratch_shapes=[
                pltpu.VMEM((16, HALF), BF),
                pltpu.VMEM((8, TOK), F32),
                pltpu.VMEM((32, HALF), BF),
                pltpu.VMEM((2 * SB, HID), F32),
                pltpu.VMEM((CHIPS, 2, 16, HALF), BF),
                pltpu.VMEM((CHIPS, 8, TOK), F32),
                pltpu.VMEM((2, 32, HALF), BF),
                pltpu.VMEM((chan, TOK), F32),
                pltpu.VMEM((chan, HID), F32),
                pltpu.VMEM((chan, HID), BF),
                pltpu.VMEM((3, 2, 3, HID, 128), BF),
                pltpu.VMEM((2, 3, 128, 2 * TOK), BF),
                pltpu.VMEM((2, 3, HID, 2 * TOK), F32),
                pltpu.VMEM((2, 3, HID, 2 * TOK), BF),
                pltpu.VMEM((CHIPS + 1, SB, chan, TOK), F32),
                pltpu.VMEM((CHIPS + 1, chan, TOK), F32),
                pltpu.VMEM((2, chan, TOK), F32),
                dma((CHIPS,)), dma((CHIPS,)), dma, dma((CHIPS,)), dma((CHIPS,)), dma, dma,
                dma((3, 2)), dma((3, 2)), dma((CHIPS,)), dma((CHIPS,)), dma((CHIPS,)), dma, dma((CHIPS,)), dma, dma, dma,
                pltpu.VMEM((batch, chan, tokens), F32), dma,
            ],
            compiler_params=pltpu.CompilerParams(has_side_effects=True, vmem_limit_bytes=60 * 2 ** 20),
            name='sweeps',
        )(mod_scale, mod_shift, w_up, w_down.T, step_size, x0)
        tile = 2048

        def fast():
            out = pl.pallas_call(
                sum_kernel,
                grid=(batch, tokens // tile),
                out_shape=jax.ShapeDtypeStruct((SB, batch, chan, tokens), F32),
                in_specs=[pl.BlockSpec((SB - 1, None, chan, tile), lambda b, i: (0, b, 0, i)),
                          pl.BlockSpec((None, chan, tile), lambda b, i: (b, 0, i))],
                out_specs=pl.BlockSpec((SB, None, chan, tile), lambda b, i: (0, b, 0, i)),
                name='sums',
            )(r, base)
            return jnp.swapaxes(out, 2, 3)

        def slow():
            return plain(x_init, w_up, w_down, mod_scale, mod_shift, step_size)

        return lax.cond(flag[0, 0] > 0.5, fast, slow)

    return jax.shard_map(device_body, mesh=mesh, in_specs=(P('data', None, None), P(None, 'model'), P('model', None), P('time', 'model'), P('time', 'model'), P('time')), out_specs=P('time', 'data', None, None), check_vma=False)
```

```python
import functools
import math

import jax
import jax.numpy as jnp
from jax import lax
from jax.experimental import pallas as pl
from jax.experimental.pallas import tpu as pltpu
from jax.sharding import PartitionSpec as P

MESH = pl.DeviceIdType.MESH
BF = jnp.bfloat16
F32 = jnp.float32
CHIPS = 64
SB = 6
HID = 1152
HALF = 640
TOK = 128
GC = math.sqrt(2.0 / math.pi)
G1 = 2.0 * GC
G2 = 8.0 * 0.044715 * GC
CW = 384
PAIRS = CHIPS // 2


def half_gelu(v):
    return v * jnp.tanh(v * (G1 + G2 * (v * v))) + v


def shift_chip(t, k, sign):
    return lax.rem(jnp.int32(t + sign * k + CHIPS), jnp.int32(CHIPS))


def main_kernel(scale, shift, up, down, hs, x0_hbm, r_out, base_out, lhs_hbm, flag,
                mods, steps, wts, gmax, gat, hst, wgt, x0, w1, w2, lh, rx, pre, act, fbuf, bas, run,
                gsem, hsem, wsem, gsend, hsend, wsend, xsem, osem, lsem, fsend, psend, bsend, bsib, rsem, psem, bsem, bpsem, xall, xallsem):
    t = lax.axis_index('time')
    p = lax.axis_index('model')
    q = 1 - p
    row = 2 * p + lax.div(t, jnp.int32(32))
    col = pl.multiple_of(lax.rem(t, jnp.int32(32)) * TOK, TOK)

    def dev(tt, pp):
        return {'time': tt, 'model': pp}

    cp_x = pltpu.make_async_copy(x0_hbm.at[row, :, pl.ds(col, TOK)], x0, xsem)
    cp_x.start()
    cp_all = pltpu.make_async_copy(x0_hbm, xall, xallsem)
    cp_all.start()

    def spread(a):
        tail = a[:, 512:]
        z = jnp.zeros_like(tail)
        last = jnp.where(p == 0, jnp.concatenate([tail, z], axis=1), jnp.concatenate([z, tail], axis=1))
        return jnp.concatenate([a[:, :512], last], axis=1)

    mods[...] = spread(jnp.concatenate([scale[...].astype(F32), shift[...].astype(F32), jnp.zeros((4, scale.shape[1]), F32)], axis=0)).astype(BF)
    for j in range(SB):
        steps[j:j + 1, :] = jnp.full((1, TOK), hs[j], F32)
    steps[SB:8, :] = jnp.zeros((2, TOK), F32)
    wts[0:16, :] = spread(up[...].astype(F32)).astype(BF)
    wts[16:32, :] = spread(down[...].astype(F32)).astype(BF)
    gmax[...] = jnp.zeros(gmax.shape, F32)
    pltpu.make_async_copy(mods, gat.at[0, p], gsem.at[0]).start()
    pltpu.make_async_copy(steps, hst.at[0], hsem.at[0]).start()
    pltpu.make_async_copy(wts, wgt.at[p], wsem).start()
    cp_w = pltpu.make_async_remote_copy(wts, wgt.at[p], wsend, wsem, device_id=dev(t, q), device_id_type=MESH)
    cp_w.start()
    cp_g0 = pltpu.make_async_remote_copy(mods, gat.at[0, p], gsend.at[0], gsem.at[0], device_id=dev(t, q), device_id_type=MESH)
    cp_g0.start()

    def send_mods(k, carry):
        d = shift_chip(t, k, -1)
        for c in range(2):
            pltpu.make_async_remote_copy(mods, gat.at[k, p], gsend.at[k], gsem.at[k], device_id=dev(d, c), device_id_type=MESH).start()
        pltpu.make_async_remote_copy(steps, hst.at[k], hsend.at[k], hsem.at[k], device_id=dev(d, p), device_id_type=MESH).start()
        return carry

    lax.fori_loop(1, CHIPS, send_mods, 0)

    zero = jnp.zeros((16, TOK), BF)
    ones_row = jnp.where(lax.broadcasted_iota(jnp.int32, (16, TOK), 0) == 0, 1.0, 0.0).astype(BF)
    for b in range(2):
        for pr in range(3):
            for r in range(8):
                for m in range(2):
                    rx[b, pr, 16 * r:16 * r + 16, TOK * m:TOK * m + TOK] = ones_row if r == 4 * m + 3 else zero
    act[1] = jnp.zeros(act.shape[1:], BF)
    pltpu.make_async_copy(wgt, wgt, wsem).wait()
    wf = wgt[...].astype(F32)

    def merged(a, b):
        return jnp.concatenate([a[:, :512], b[:, :512], a[:, 512:] + b[:, 512:]], axis=1)

    w1[...] = merged(wf[0, :16], wf[1, :16])
    w2[...] = merged(wf[0, 16:], wf[1, 16:]).astype(BF)
    cp_x.wait()

    first = lax.broadcasted_iota(jnp.int32, (16, HID), 0) == 0

    def build(k, slot, half):
        mf = merged(gat[k, 0].astype(F32), gat[k, 1].astype(F32))
        w = w1[...]
        gmax[...] = jnp.maximum(gmax[...], jnp.abs(mf[:12]))
        for pr in range(3):
            parts = []
            for m in range(2):
                j = 2 * pr + m
                ws = w * (0.5 * mf[j:j + 1] + 0.5)
                hi = ws.astype(BF)
                rest = ws - hi.astype(F32)
                mid = rest.astype(BF)
                low = (rest - mid.astype(F32)).astype(BF)
                bias = jnp.where(first, 0.5 * mf[SB + j:SB + j + 1], 0.0).astype(BF)
                parts += [hi, mid, low, bias]
            full = jnp.concatenate(parts, axis=0)
            for c in range(0, HID, 128):
                lh[slot, half, pr, c:c + 128, :] = full[:, c:c + 128].T

    def put_x(b, j, x):
        xb = x.astype(BF)
        pr, m = j // 2, j % 2
        for r in range(3):
            rx[b, pr, 64 * m + 16 * r:64 * m + 16 * r + 16, TOK * m:TOK * m + TOK] = xb

    def rx_prefix(b, s, c):
        for j in range(SB):
            put_x(b, j, s)
            s = s + fbuf[c, j]
        return s

    def body(cur, slot, half, finish, skip=False):
        def mm1(pr, lo):
            pre[1 - cur, pr, lo:lo + CW, :] = jnp.dot(lh[slot, half, pr, lo:lo + CW, :], rx[1 - cur, pr], preferred_element_type=F32)
        rows = []
        for pr in range(3):
            acc = jnp.zeros((16, 2 * TOK), F32)
            for lo in range(0, HID, CW):
                if not skip:
                    mm1(pr, lo)
                acc = acc + jnp.dot(w2[:, lo:lo + CW], act[1 - cur, pr, lo:lo + CW, :], preferred_element_type=F32)
                act[cur, pr, lo:lo + CW, :] = half_gelu(pre[cur, pr, lo:lo + CW, :]).astype(BF)
            rows += [acc[:, :TOK], acc[:, TOK:]]
        finish(rows)

    def tail(cur, finish):
        rows = []
        for pr in range(3):
            acc = jnp.dot(w2[...], act[cur, pr], preferred_element_type=F32)
            rows += [acc[:, :TOK], acc[:, TOK:]]
        finish(rows)

    def head(slot):
        for pr in range(3):
            for lo in range(0, HID, CW):
                pre[0, pr, lo:lo + CW, :] = jnp.dot(lh[slot, 0, pr, lo:lo + CW, :], rx[0, pr], preferred_element_type=F32)

    def store_f(c, kk, rows):
        tot = None
        for j in range(SB):
            f = hst[kk, j:j + 1, :] * rows[j]
            fbuf[c, j] = f
            tot = f if tot is None else tot + f
        return tot

    def wait_mods(k):
        pltpu.make_async_copy(gat.at[k], gat.at[k], gsem.at[k]).wait()
        pltpu.make_async_copy(hst.at[k], hst.at[k], hsem.at[k]).wait()

    def out_lh(g, half):
        return pltpu.make_async_copy(lh.at[g % 3, half], lhs_hbm.at[shift_chip(t, 2 * g + half, 1)], osem.at[g % 3, half])

    for g in range(2):
        for half in range(2):
            pltpu.make_async_copy(lh.at[g + 1, half], lhs_hbm.at[CHIPS + 2 * g + half], osem.at[g + 1, half]).start()
    for half in range(2):
        wait_mods(half)
        build(half, 0, half)
    for j in range(SB):
        put_x(0, j, x0[...])
        put_x(1, j, x0[...])
    head(0)

    def step0(i, more):
        for half in range(2):
            pltpu.make_async_copy(lh.at[(i + 1) % 3, half], lhs_hbm.at[half], osem.at[(i + 1) % 3, half]).wait()
            out_lh(i, half).start()
            if more:
                wait_mods(2 * i + 2 + half)
        for u in range(2):
            n = 2 * i + u
            if more:
                build(n + 2, (i + 1) % 3, u)
            prev = jnp.maximum(n - 1, 0)
            where = jnp.where(n == 0, CHIPS, shift_chip(t, prev, 1))
            body(u, (i + u) % 3, 1 - u, lambda rows: store_f(where, prev, rows), skip=(u == 1 and not more))

    def loop0(i, carry):
        step0(i, True)
        return carry

    lax.fori_loop(0, PAIRS - 1, loop0, 0)
    step0(PAIRS - 1, False)
    tail(1, lambda rows: store_f(shift_chip(t, CHIPS - 1, 1), CHIPS - 1, rows))
    for g in (PAIRS - 2, PAIRS - 1):
        for half in range(2):
            out_lh(g, half).wait()

    def top(a):
        return jnp.max(jnp.max(a, axis=1, keepdims=True), axis=0, keepdims=True)

    wa = jnp.abs(w1[...])
    wtop = top(wa)
    wlow = -top(-jnp.where(wa == 0.0, 1.0, wa))
    gtop = 1.0 + top(gmax[0:SB])
    btop = top(gmax[SB:2 * SB])
    dtop = top(jnp.abs(w2[...].astype(F32)))
    habs = lax.fori_loop(0, CHIPS, lambda k, a: a + jnp.abs(hst[k]), jnp.zeros((8, TOK), F32))
    hsum = 8.0 * top(habs)
    cp_all.wait()
    xtop = top(jnp.max(jnp.abs(xall[...]), axis=0))
    bound = xtop
    for _ in range(4):
        arg = 16.0 * bound * (1.0 + wtop) * gtop + btop
        bound = xtop + hsum * (HID * 2.0) * dtop * arg
    safe = (16.0 * bound * (1.0 + wtop) * gtop < 2.0 ** 100) & (wlow > 2.0 ** -80)
    flag[...] = jnp.broadcast_to(jnp.where(safe, 1.0, 0.0), (8, TOK))

    def block_of(s, n):
        if s < 3:
            return n
        return shift_chip(t, lax.rem(jnp.int32(n + 1), jnp.int32(CHIPS)), 1)

    def in_lh(block, g, half):
        return pltpu.make_async_copy(lhs_hbm.at[block], lh.at[g % 3, half], lsem.at[g % 3, half])

    def send_f(k):
        c = shift_chip(t, k, 1)
        pltpu.make_async_remote_copy(fbuf.at[c, pl.ds(0, SB - 1)], r_out.at[:, row, :, pl.ds(col, TOK)],
                                     fsend.at[k], rsem, device_id=dev(c, p), device_id_type=MESH).start()

    for g in range(2):
        for half in range(2):
            in_lh(2 * g + half, g, half).start()
    for half in range(2):
        in_lh(half, 0, half).wait()

    for s in (1, 2, 3):
        base = PAIRS * (s - 1)
        for b in range(2):
            if s < 3:
                run[0] = rx_prefix(b, run[0] if b else x0[...], b)
            else:
                rx_prefix(b, bas[block_of(3, b)], block_of(3, b))
            if b == 0:
                head(base % 3)

        def step(i, send, s=s, base=base):
            g = base + i
            for half in range(2):
                in_lh(0, g + 1, half).wait()
            for half in range(2):
                n = 2 * i + 4 + half
                wrap = lax.rem(n, jnp.int32(CHIPS))
                nxt = block_of(min(s + 1, 3), wrap)
                in_lh(jnp.where(n < CHIPS, block_of(s, wrap), nxt), g + 2, half).start()
            if send:
                send_f(2 * i - 2)
                send_f(2 * i - 1)
            for u in range(2):
                n = 2 * i + u
                nx = jnp.minimum(n + 2, CHIPS - 1)
                prev = jnp.maximum(n - 1, 0)
                cp = block_of(s, prev)
                where = jnp.where(n == 0, CHIPS, cp)
                kk = shift_chip(cp, t, -1)

                def finish(rows):
                    tot = store_f(where, kk, rows)
                    if s == 2:
                        bas[where] = run[1]
                        run[1] = jnp.where(n == 0, x0[...], run[1] + tot)
                    if s == 3:
                        bas[where] = tot
                body(u, (g + u) % 3, 1 - u, finish)
                if s < 3:
                    run[0] = rx_prefix(u, run[0], nx)
                else:
                    cn = block_of(3, nx)
                    rx_prefix(u, bas[cn], cn)

        def loop(i, carry, step=step):
            step(i, False)
            return carry

        def loop_send(i, carry, step=step):
            step(i, True)
            return carry

        if s < 3:
            lax.fori_loop(0, PAIRS, loop, 0)
        else:
            lax.fori_loop(0, 2, loop, 0)
            send_f(1)
            lax.fori_loop(2, PAIRS, loop_send, 0)

        last = block_of(s, CHIPS - 1)

        def finish_last(rows, s=s, last=last):
            tot = store_f(last, shift_chip(last, t, -1) if s < 3 else 0, rows)
            if s == 2:
                bas[last] = run[1]
            if s == 3:
                bas[last] = tot
        tail(1, finish_last)

    send_f(CHIPS - 2)
    send_f(CHIPS - 1)
    for half in range(2):
        in_lh(0, 3 * PAIRS + 1, half).wait()
    mine = r_out.at[:, row, :, pl.ds(col, TOK)]
    own_f = pltpu.make_async_copy(fbuf.at[t, pl.ds(0, SB - 1)], mine, rsem)
    own_f.start()

    def scan_base(c, s):
        tot = bas[c]
        bas[c] = s
        return s + tot

    lax.fori_loop(0, CHIPS, scan_base, x0[...])

    def send_b(k, carry):
        c = shift_chip(t, k, 1)
        pltpu.make_async_remote_copy(bas.at[c], base_out.at[row, :, pl.ds(col, TOK)],
                                     bsend.at[k], bsem, device_id=dev(c, p), device_id_type=MESH).start()
        return carry

    lax.fori_loop(1, CHIPS, send_b, 0)
    pltpu.make_async_copy(bas.at[t], base_out.at[row, :, pl.ds(col, TOK)], bsem).start()

    half_r = r_out.at[:, pl.ds(2 * p, 2)]
    pltpu.make_async_copy(half_r, half_r, rsem).wait()
    sib_f = pltpu.make_async_remote_copy(half_r, half_r, psend, psem, device_id=dev(t, q), device_id_type=MESH)
    sib_f.start()
    half_b = base_out.at[pl.ds(2 * p, 2)]
    pltpu.make_async_copy(half_b, half_b, bsem).wait()
    sib_b = pltpu.make_async_remote_copy(half_b, half_b, bsib, bpsem, device_id=dev(t, q), device_id_type=MESH)
    sib_b.start()

    cp_w.wait_send()
    cp_g0.wait_send()

    def drain(k, carry):
        pltpu.make_async_copy(gat.at[k], gat.at[k], gsend.at[k]).wait()
        pltpu.make_async_copy(hst.at[k], hst.at[k], hsend.at[k]).wait()
        pltpu.make_async_copy(fbuf.at[k, pl.ds(0, SB - 1)], fbuf.at[k, pl.ds(0, SB - 1)], fsend.at[k]).wait()
        pltpu.make_async_copy(bas.at[k], bas.at[k], bsend.at[k]).wait()
        return carry

    lax.fori_loop(1, CHIPS, drain, 0)
    sib_f.wait_send()
    sib_b.wait_send()
    theirs = r_out.at[:, pl.ds(2 * q, 2)]
    pltpu.make_async_copy(theirs, theirs, psem).wait()
    half_q = base_out.at[pl.ds(2 * q, 2)]
    pltpu.make_async_copy(half_q, half_q, bpsem).wait()


def sum_kernel(r_ref, b_ref, o_ref):
    s = b_ref[...]
    o_ref[0] = s
    for j in range(SB - 1):
        s = s + r_ref[j]
        o_ref[j + 1] = s


def plain(x_init, w_up, w_down, mod_scale, mod_shift, step_size):
    time_devs = lax.axis_size('time')
    scale_f = 1.0 + mod_scale.astype(F32)
    shift_f = mod_shift.astype(F32)
    step_col = step_size[:, None, None, None]

    def drift(args):
        lat, sc, sh = args
        act = jnp.einsum('bnc,cd->bnd', lat.astype(BF), w_up, preferred_element_type=F32)
        hidden = jax.nn.gelu(act * sc + sh, approximate=True)
        return jnp.einsum('bnd,dc->bnc', hidden.astype(BF), w_down, preferred_element_type=F32)

    def sweep(_, latents):
        part = lax.map(drift, (latents, scale_f, shift_f))
        drifts = step_col * (part + lax.ppermute(part, 'model', [(0, 1), (1, 0)]))
        running = jnp.cumsum(drifts, axis=0)
        total = running[-1]
        acc = total
        hop = 1
        while hop < time_devs:
            acc = acc + lax.ppermute(acc, 'time', [(a, a + hop) for a in range(time_devs - hop)])
            hop = hop * 2
        return (x_init + (acc - total))[None] + (running - drifts)

    start = jnp.broadcast_to(x_init[None], (mod_scale.shape[0],) + x_init.shape)
    return lax.fori_loop(0, 4, sweep, start)


def solution(mesh):
    def device_body(x_init, w_up, w_down, mod_scale, mod_shift, step_size):
        batch, tokens, chan = x_init.shape
        x0 = jnp.swapaxes(x_init, 1, 2)
        vm = pl.BlockSpec(memory_space=pltpu.VMEM)
        sm = pl.BlockSpec(memory_space=pltpu.SMEM)
        hb = pl.BlockSpec(memory_space=pl.ANY)
        dma = pltpu.SemaphoreType.DMA
        r, base, _, flag = pl.pallas_call(
            main_kernel,
            out_shape=(
                jax.ShapeDtypeStruct((SB - 1, batch, chan, tokens), F32),
                jax.ShapeDtypeStruct((batch, chan, tokens), F32),
                jax.ShapeDtypeStruct((CHIPS + 4, 3, HID, 128), BF),
                jax.ShapeDtypeStruct((8, TOK), F32),
            ),
            in_specs=[vm, vm, vm, vm, sm, hb],
            out_specs=(hb, hb, hb, vm),
            scratch_shapes=[
                pltpu.VMEM((16, HALF), BF),
                pltpu.VMEM((8, TOK), F32),
                pltpu.VMEM((32, HALF), BF),
                pltpu.VMEM((2 * SB, HID), F32),
                pltpu.VMEM((CHIPS, 2, 16, HALF), BF),
                pltpu.VMEM((CHIPS, 8, TOK), F32),
                pltpu.VMEM((2, 32, HALF), BF),
                pltpu.VMEM((chan, TOK), F32),
                pltpu.VMEM((chan, HID), F32),
                pltpu.VMEM((chan, HID), BF),
                pltpu.VMEM((3, 2, 3, HID, 128), BF),
                pltpu.VMEM((2, 3, 128, 2 * TOK), BF),
                pltpu.VMEM((2, 3, HID, 2 * TOK), F32),
                pltpu.VMEM((2, 3, HID, 2 * TOK), BF),
                pltpu.VMEM((CHIPS + 1, SB, chan, TOK), F32),
                pltpu.VMEM((CHIPS + 1, chan, TOK), F32),
                pltpu.VMEM((2, chan, TOK), F32),
                dma((CHIPS,)), dma((CHIPS,)), dma, dma((CHIPS,)), dma((CHIPS,)), dma, dma,
                dma((3, 2)), dma((3, 2)), dma((CHIPS,)), dma, dma((CHIPS,)), dma, dma, dma, dma, dma,
                pltpu.VMEM((batch, chan, tokens), F32), dma,
            ],
            compiler_params=pltpu.CompilerParams(has_side_effects=True, vmem_limit_bytes=60 * 2 ** 20),
            name='sweeps',
        )(mod_scale, mod_shift, w_up, w_down.T, step_size, x0)
        tile = 2048

        def fast():
            out = pl.pallas_call(
                sum_kernel,
                grid=(batch, tokens // tile),
                out_shape=jax.ShapeDtypeStruct((SB, batch, chan, tokens), F32),
                in_specs=[pl.BlockSpec((SB - 1, None, chan, tile), lambda b, i: (0, b, 0, i)),
                          pl.BlockSpec((None, chan, tile), lambda b, i: (b, 0, i))],
                out_specs=pl.BlockSpec((SB, None, chan, tile), lambda b, i: (0, b, 0, i)),
                name='sums',
            )(r, base)
            return jnp.swapaxes(out, 2, 3)

        def slow():
            return plain(x_init, w_up, w_down, mod_scale, mod_shift, step_size)

        return lax.cond(flag[0, 0] > 0.5, fast, slow)

    return jax.shard_map(device_body, mesh=mesh, in_specs=(P('data', None, None), P(None, 'model'), P('model', None), P('time', 'model'), P('time', 'model'), P('time')), out_specs=P('time', 'data', None, None), check_vma=False)
```

```python
import functools
import math

import jax
import jax.numpy as jnp
from jax import lax
from jax.experimental import pallas as pl
from jax.experimental.pallas import tpu as pltpu
from jax.sharding import PartitionSpec as P

MESH = pl.DeviceIdType.MESH
BF = jnp.bfloat16
F32 = jnp.float32
CHIPS = 64
SB = 6
HID = 1152
HALF = 640
TOK = 128
GC = math.sqrt(2.0 / math.pi)
G1 = 2.0 * GC
G2 = 8.0 * 0.044715 * GC
CW = 384
PAIRS = CHIPS // 2


def half_gelu(v):
    return v * jnp.tanh(v * (G1 + G2 * (v * v))) + v


def shift_chip(t, k, sign):
    return lax.rem(jnp.int32(t + sign * k + CHIPS), jnp.int32(CHIPS))


def main_kernel(scale, shift, up, down, hs, x0_hbm, r_out, base_out, lhs_hbm, flag,
                mods, steps, wts, gmax, gat, hst, wgt, x0, w1, w2, lh, rx, pre, act, fbuf, bas, run,
                gsem, hsem, wsem, gsend, hsend, wsend, xsem, osem, lsem, fsend, psend, bsend, bsib, rsem, psem, bsem, bpsem, xall, xallsem):
    t = lax.axis_index('time')
    p = lax.axis_index('model')
    q = 1 - p
    row = 2 * p + lax.div(t, jnp.int32(32))
    col = pl.multiple_of(lax.rem(t, jnp.int32(32)) * TOK, TOK)

    def dev(tt, pp):
        return {'time': tt, 'model': pp}

    cp_x = pltpu.make_async_copy(x0_hbm.at[row, :, pl.ds(col, TOK)], x0, xsem)
    cp_x.start()
    cp_all = pltpu.make_async_copy(x0_hbm, xall, xallsem)
    cp_all.start()

    def spread(a):
        tail = a[:, 512:]
        z = jnp.zeros_like(tail)
        last = jnp.where(p == 0, jnp.concatenate([tail, z], axis=1), jnp.concatenate([z, tail], axis=1))
        return jnp.concatenate([a[:, :512], last], axis=1)

    mods[...] = spread(jnp.concatenate([scale[...].astype(F32), shift[...].astype(F32), jnp.zeros((4, scale.shape[1]), F32)], axis=0)).astype(BF)
    for j in range(SB):
        steps[j:j + 1, :] = jnp.full((1, TOK), hs[j], F32)
    steps[SB:8, :] = jnp.zeros((2, TOK), F32)
    wts[0:16, :] = spread(up[...].astype(F32)).astype(BF)
    wts[16:32, :] = spread(down[...].astype(F32)).astype(BF)
    gmax[...] = jnp.zeros(gmax.shape, F32)
    zero = jnp.zeros((16, TOK), BF)
    ones_row = jnp.where(lax.broadcasted_iota(jnp.int32, (16, TOK), 0) == 0, 1.0, 0.0).astype(BF)
    for b in range(2):
        for pr in range(3):
            for r in range(8):
                for m in range(2):
                    rx[b, pr, 16 * r:16 * r + 16, TOK * m:TOK * m + TOK] = ones_row if r == 4 * m + 3 else zero
    act[1] = jnp.zeros(act.shape[1:], BF)
    pltpu.make_async_copy(mods, gat.at[0, p], gsem.at[0]).start()
    pltpu.make_async_copy(steps, hst.at[0], hsem.at[0]).start()
    pltpu.make_async_copy(wts, wgt.at[p], wsem).start()
    cp_w = pltpu.make_async_remote_copy(wts, wgt.at[p], wsend, wsem, device_id=dev(t, q), device_id_type=MESH)
    cp_w.start()
    cp_g0 = pltpu.make_async_remote_copy(mods, gat.at[0, p], gsend.at[0], gsem.at[0], device_id=dev(t, q), device_id_type=MESH)
    cp_g0.start()

    def send_mods(k, carry):
        d = shift_chip(t, k, -1)
        for c in range(2):
            pltpu.make_async_remote_copy(mods, gat.at[k, p], gsend.at[k], gsem.at[k], device_id=dev(d, c), device_id_type=MESH).start()
        pltpu.make_async_remote_copy(steps, hst.at[k], hsend.at[k], hsem.at[k], device_id=dev(d, p), device_id_type=MESH).start()
        return carry

    lax.fori_loop(1, CHIPS, send_mods, 0)

    pltpu.make_async_copy(wgt, wgt, wsem).wait()
    wf = wgt[...].astype(F32)

    def merged(a, b):
        return jnp.concatenate([a[:, :512], b[:, :512], a[:, 512:] + b[:, 512:]], axis=1)

    w1[...] = merged(wf[0, :16], wf[1, :16])
    w2[...] = merged(wf[0, 16:], wf[1, 16:]).astype(BF)
    cp_x.wait()

    first = lax.broadcasted_iota(jnp.int32, (16, HID), 0) == 0

    def build(k, slot, half):
        mf = merged(gat[k, 0].astype(F32), gat[k, 1].astype(F32))
        w = w1[...]
        gmax[...] = jnp.maximum(gmax[...], jnp.abs(mf[:12]))
        for pr in range(3):
            parts = []
            for m in range(2):
                j = 2 * pr + m
                ws = w * (0.5 * mf[j:j + 1] + 0.5)
                hi = ws.astype(BF)
                rest = ws - hi.astype(F32)
                mid = rest.astype(BF)
                low = (rest - mid.astype(F32)).astype(BF)
                bias = jnp.where(first, 0.5 * mf[SB + j:SB + j + 1], 0.0).astype(BF)
                parts += [hi, mid, low, bias]
            full = jnp.concatenate(parts, axis=0)
            for c in range(0, HID, 128):
                lh[slot, half, pr, c:c + 128, :] = full[:, c:c + 128].T

    def put_x(b, j, x):
        xb = x.astype(BF)
        pr, m = j // 2, j % 2
        for r in range(3):
            rx[b, pr, 64 * m + 16 * r:64 * m + 16 * r + 16, TOK * m:TOK * m + TOK] = xb

    def rx_prefix(b, s, c):
        for j in range(SB):
            put_x(b, j, s)
            s = s + fbuf[c, j]
        return s

    def body(cur, slot, half, finish, skip=False):
        def mm1(pr, lo):
            pre[1 - cur, pr, lo:lo + CW, :] = jnp.dot(lh[slot, half, pr, lo:lo + CW, :], rx[1 - cur, pr], preferred_element_type=F32)
        rows = []
        for pr in range(3):
            acc = jnp.zeros((16, 2 * TOK), F32)
            for lo in range(0, HID, CW):
                if not skip:
                    mm1(pr, lo)
                acc = acc + jnp.dot(w2[:, lo:lo + CW], act[1 - cur, pr, lo:lo + CW, :], preferred_element_type=F32)
                act[cur, pr, lo:lo + CW, :] = half_gelu(pre[cur, pr, lo:lo + CW, :]).astype(BF)
            rows += [acc[:, :TOK], acc[:, TOK:]]
        finish(rows)

    def tail(cur, finish):
        rows = []
        for pr in range(3):
            acc = jnp.dot(w2[...], act[cur, pr], preferred_element_type=F32)
            rows += [acc[:, :TOK], acc[:, TOK:]]
        finish(rows)

    def head(slot):
        for pr in range(3):
            for lo in range(0, HID, CW):
                pre[0, pr, lo:lo + CW, :] = jnp.dot(lh[slot, 0, pr, lo:lo + CW, :], rx[0, pr], preferred_element_type=F32)

    def store_f(c, kk, rows):
        tot = None
        for j in range(SB):
            f = hst[kk, j:j + 1, :] * rows[j]
            fbuf[c, j] = f
            tot = f if tot is None else tot + f
        return tot

    def wait_mods(k):
        pltpu.make_async_copy(gat.at[k], gat.at[k], gsem.at[k]).wait()
        pltpu.make_async_copy(hst.at[k], hst.at[k], hsem.at[k]).wait()

    def out_lh(g, half):
        return pltpu.make_async_copy(lh.at[g % 3, half], lhs_hbm.at[shift_chip(t, 2 * g + half, 1)], osem.at[g % 3, half])

    for g in range(2):
        for half in range(2):
            pltpu.make_async_copy(lh.at[g + 1, half], lhs_hbm.at[CHIPS + 2 * g + half], osem.at[g + 1, half]).start()
    for half in range(2):
        wait_mods(half)
        build(half, 0, half)
    for j in range(SB):
        put_x(0, j, x0[...])
        put_x(1, j, x0[...])
    head(0)

    def step0(i, more):
        for half in range(2):
            pltpu.make_async_copy(lh.at[(i + 1) % 3, half], lhs_hbm.at[half], osem.at[(i + 1) % 3, half]).wait()
            out_lh(i, half).start()
            if more:
                wait_mods(2 * i + 2 + half)
        for u in range(2):
            n = 2 * i + u
            if more:
                build(n + 2, (i + 1) % 3, u)
            prev = jnp.maximum(n - 1, 0)
            where = jnp.where(n == 0, CHIPS, shift_chip(t, prev, 1))
            body(u, (i + u) % 3, 1 - u, lambda rows: store_f(where, prev, rows), skip=(u == 1 and not more))

    def loop0(i, carry):
        step0(i, True)
        return carry

    lax.fori_loop(0, PAIRS - 1, loop0, 0)
    step0(PAIRS - 1, False)
    tail(1, lambda rows: store_f(shift_chip(t, CHIPS - 1, 1), CHIPS - 1, rows))
    for g in (PAIRS - 2, PAIRS - 1):
        for half in range(2):
            out_lh(g, half).wait()

    def top(a):
        return jnp.max(jnp.max(a, axis=1, keepdims=True), axis=0, keepdims=True)

    wa = jnp.abs(w1[...])
    wtop = top(wa)
    wlow = -top(-jnp.where(wa == 0.0, 1.0, wa))
    gtop = 1.0 + top(gmax[0:SB])
    btop = top(gmax[SB:2 * SB])
    dtop = top(jnp.abs(w2[...].astype(F32)))
    habs = lax.fori_loop(0, CHIPS, lambda k, a: a + jnp.abs(hst[k]), jnp.zeros((8, TOK), F32))
    hsum = 8.0 * top(habs)
    cp_all.wait()
    xtop = top(jnp.max(jnp.abs(xall[...]), axis=0))
    bound = xtop
    for _ in range(4):
        arg = 16.0 * bound * (1.0 + wtop) * gtop + btop
        bound = xtop + hsum * (HID * 2.0) * dtop * arg
    safe = (16.0 * bound * (1.0 + wtop) * gtop < 2.0 ** 100) & (wlow > 2.0 ** -80)
    flag[...] = jnp.broadcast_to(jnp.where(safe, 1.0, 0.0), (8, TOK))

    def block_of(s, n):
        if s < 3:
            return n
        return shift_chip(t, lax.rem(jnp.int32(n + 1), jnp.int32(CHIPS)), 1)

    def in_lh(block, g, half):
        return pltpu.make_async_copy(lhs_hbm.at[block], lh.at[g % 3, half], lsem.at[g % 3, half])

    def send_f(k):
        c = shift_chip(t, k, 1)
        pltpu.make_async_remote_copy(fbuf.at[c, pl.ds(0, SB - 1)], r_out.at[:, row, :, pl.ds(col, TOK)],
                                     fsend.at[k], rsem, device_id=dev(c, p), device_id_type=MESH).start()

    for g in range(2):
        for half in range(2):
            in_lh(2 * g + half, g, half).start()
    for half in range(2):
        in_lh(half, 0, half).wait()

    for s in (1, 2, 3):
        base = PAIRS * (s - 1)
        for b in range(2):
            if s < 3:
                run[0] = rx_prefix(b, run[0] if b else x0[...], b)
            else:
                rx_prefix(b, bas[block_of(3, b)], block_of(3, b))
            if b == 0:
                head(base % 3)

        def step(i, send, s=s, base=base):
            g = base + i
            for half in range(2):
                in_lh(0, g + 1, half).wait()
            for half in range(2):
                n = 2 * i + 4 + half
                wrap = lax.rem(n, jnp.int32(CHIPS))
                nxt = block_of(min(s + 1, 3), wrap)
                in_lh(jnp.where(n < CHIPS, block_of(s, wrap), nxt), g + 2, half).start()
            if send:
                send_f(2 * i - 2)
                send_f(2 * i - 1)
            for u in range(2):
                n = 2 * i + u
                nx = jnp.minimum(n + 2, CHIPS - 1)
                prev = jnp.maximum(n - 1, 0)
                cp = block_of(s, prev)
                where = jnp.where(n == 0, CHIPS, cp)
                kk = shift_chip(cp, t, -1)

                def finish(rows):
                    tot = store_f(where, kk, rows)
                    if s == 2:
                        bas[where] = run[1]
                        run[1] = jnp.where(n == 0, x0[...], run[1] + tot)
                    if s == 3:
                        bas[where] = tot
                body(u, (g + u) % 3, 1 - u, finish)
                if s < 3:
                    run[0] = rx_prefix(u, run[0], nx)
                else:
                    cn = block_of(3, nx)
                    rx_prefix(u, bas[cn], cn)

        def loop(i, carry, step=step):
            step(i, False)
            return carry

        def loop_send(i, carry, step=step):
            step(i, True)
            return carry

        if s < 3:
            lax.fori_loop(0, PAIRS, loop, 0)
        else:
            lax.fori_loop(0, 2, loop, 0)
            send_f(1)
            lax.fori_loop(2, PAIRS, loop_send, 0)

        last = block_of(s, CHIPS - 1)

        def finish_last(rows, s=s, last=last):
            tot = store_f(last, shift_chip(last, t, -1) if s < 3 else 0, rows)
            if s == 2:
                bas[last] = run[1]
            if s == 3:
                bas[last] = tot
        tail(1, finish_last)

    send_f(CHIPS - 2)
    send_f(CHIPS - 1)
    for half in range(2):
        in_lh(0, 3 * PAIRS + 1, half).wait()
    mine = r_out.at[:, row, :, pl.ds(col, TOK)]
    own_f = pltpu.make_async_copy(fbuf.at[t, pl.ds(0, SB - 1)], mine, rsem)
    own_f.start()

    def scan_base(c, s):
        tot = bas[c]
        bas[c] = s
        return s + tot

    lax.fori_loop(0, CHIPS, scan_base, x0[...])

    def send_b(k, carry):
        c = shift_chip(t, k, 1)
        pltpu.make_async_remote_copy(bas.at[c], base_out.at[row, :, pl.ds(col, TOK)],
                                     bsend.at[k], bsem, device_id=dev(c, p), device_id_type=MESH).start()
        return carry

    lax.fori_loop(1, CHIPS, send_b, 0)
    pltpu.make_async_copy(bas.at[t], base_out.at[row, :, pl.ds(col, TOK)], bsem).start()

    half_r = r_out.at[:, pl.ds(2 * p, 2)]
    pltpu.make_async_copy(half_r, half_r, rsem).wait()
    sib_f = pltpu.make_async_remote_copy(half_r, half_r, psend, psem, device_id=dev(t, q), device_id_type=MESH)
    sib_f.start()
    half_b = base_out.at[pl.ds(2 * p, 2)]
    pltpu.make_async_copy(half_b, half_b, bsem).wait()
    sib_b = pltpu.make_async_remote_copy(half_b, half_b, bsib, bpsem, device_id=dev(t, q), device_id_type=MESH)
    sib_b.start()

    cp_w.wait_send()
    cp_g0.wait_send()

    def drain(k, carry):
        pltpu.make_async_copy(gat.at[k], gat.at[k], gsend.at[k]).wait()
        pltpu.make_async_copy(hst.at[k], hst.at[k], hsend.at[k]).wait()
        pltpu.make_async_copy(fbuf.at[k, pl.ds(0, SB - 1)], fbuf.at[k, pl.ds(0, SB - 1)], fsend.at[k]).wait()
        pltpu.make_async_copy(bas.at[k], bas.at[k], bsend.at[k]).wait()
        return carry

    lax.fori_loop(1, CHIPS, drain, 0)
    sib_f.wait_send()
    sib_b.wait_send()
    theirs = r_out.at[:, pl.ds(2 * q, 2)]
    pltpu.make_async_copy(theirs, theirs, psem).wait()
    half_q = base_out.at[pl.ds(2 * q, 2)]
    pltpu.make_async_copy(half_q, half_q, bpsem).wait()


def sum_kernel(r_ref, b_ref, o_ref):
    s = b_ref[...]
    o_ref[0] = s
    for j in range(SB - 1):
        s = s + r_ref[j]
        o_ref[j + 1] = s


def plain(x_init, w_up, w_down, mod_scale, mod_shift, step_size):
    time_devs = lax.axis_size('time')
    scale_f = 1.0 + mod_scale.astype(F32)
    shift_f = mod_shift.astype(F32)
    step_col = step_size[:, None, None, None]

    def drift(args):
        lat, sc, sh = args
        act = jnp.einsum('bnc,cd->bnd', lat.astype(BF), w_up, preferred_element_type=F32)
        hidden = jax.nn.gelu(act * sc + sh, approximate=True)
        return jnp.einsum('bnd,dc->bnc', hidden.astype(BF), w_down, preferred_element_type=F32)

    def sweep(_, latents):
        part = lax.map(drift, (latents, scale_f, shift_f))
        drifts = step_col * (part + lax.ppermute(part, 'model', [(0, 1), (1, 0)]))
        running = jnp.cumsum(drifts, axis=0)
        total = running[-1]
        acc = total
        hop = 1
        while hop < time_devs:
            acc = acc + lax.ppermute(acc, 'time', [(a, a + hop) for a in range(time_devs - hop)])
            hop = hop * 2
        return (x_init + (acc - total))[None] + (running - drifts)

    start = jnp.broadcast_to(x_init[None], (mod_scale.shape[0],) + x_init.shape)
    return lax.fori_loop(0, 4, sweep, start)


def solution(mesh):
    def device_body(x_init, w_up, w_down, mod_scale, mod_shift, step_size):
        batch, tokens, chan = x_init.shape
        x0 = jnp.swapaxes(x_init, 1, 2)
        vm = pl.BlockSpec(memory_space=pltpu.VMEM)
        sm = pl.BlockSpec(memory_space=pltpu.SMEM)
        hb = pl.BlockSpec(memory_space=pl.ANY)
        dma = pltpu.SemaphoreType.DMA
        r, base, _, flag = pl.pallas_call(
            main_kernel,
            out_shape=(
                jax.ShapeDtypeStruct((SB - 1, batch, chan, tokens), F32),
                jax.ShapeDtypeStruct((batch, chan, tokens), F32),
                jax.ShapeDtypeStruct((CHIPS + 4, 3, HID, 128), BF),
                jax.ShapeDtypeStruct((8, TOK), F32),
            ),
            in_specs=[vm, vm, vm, vm, sm, hb],
            out_specs=(hb, hb, hb, vm),
            scratch_shapes=[
                pltpu.VMEM((16, HALF), BF),
                pltpu.VMEM((8, TOK), F32),
                pltpu.VMEM((32, HALF), BF),
                pltpu.VMEM((2 * SB, HID), F32),
                pltpu.VMEM((CHIPS, 2, 16, HALF), BF),
                pltpu.VMEM((CHIPS, 8, TOK), F32),
                pltpu.VMEM((2, 32, HALF), BF),
                pltpu.VMEM((chan, TOK), F32),
                pltpu.VMEM((chan, HID), F32),
                pltpu.VMEM((chan, HID), BF),
                pltpu.VMEM((3, 2, 3, HID, 128), BF),
                pltpu.VMEM((2, 3, 128, 2 * TOK), BF),
                pltpu.VMEM((2, 3, HID, 2 * TOK), F32),
                pltpu.VMEM((2, 3, HID, 2 * TOK), BF),
                pltpu.VMEM((CHIPS + 1, SB, chan, TOK), F32),
                pltpu.VMEM((CHIPS + 1, chan, TOK), F32),
                pltpu.VMEM((2, chan, TOK), F32),
                dma((CHIPS,)), dma((CHIPS,)), dma, dma((CHIPS,)), dma((CHIPS,)), dma, dma,
                dma((3, 2)), dma((3, 2)), dma((CHIPS,)), dma, dma((CHIPS,)), dma, dma, dma, dma, dma,
                pltpu.VMEM((batch, chan, tokens), F32), dma,
            ],
            compiler_params=pltpu.CompilerParams(has_side_effects=True, vmem_limit_bytes=60 * 2 ** 20),
            name='sweeps',
        )(mod_scale, mod_shift, w_up, w_down.T, step_size, x0)
        tile = 4096

        def fast():
            out = pl.pallas_call(
                sum_kernel,
                grid=(batch, tokens // tile),
                out_shape=jax.ShapeDtypeStruct((SB, batch, chan, tokens), F32),
                in_specs=[pl.BlockSpec((SB - 1, None, chan, tile), lambda b, i: (0, b, 0, i)),
                          pl.BlockSpec((None, chan, tile), lambda b, i: (b, 0, i))],
                out_specs=pl.BlockSpec((SB, None, chan, tile), lambda b, i: (0, b, 0, i)),
                name='sums',
            )(r, base)
            return jnp.swapaxes(out, 2, 3)

        def slow():
            return plain(x_init, w_up, w_down, mod_scale, mod_shift, step_size)

        return lax.cond(flag[0, 0] > 0.5, fast, slow)

    return jax.shard_map(device_body, mesh=mesh, in_specs=(P('data', None, None), P(None, 'model'), P('model', None), P('time', 'model'), P('time', 'model'), P('time')), out_specs=P('time', 'data', None, None), check_vma=False)
```
